256 devices in a mesh: seq: 32 (over x_lo, z, core), head: 8 (over y, x_hi).
Axes of the slice: x: 4 (x_hi: 2, x_lo: 2; x = x_hi * 2 + x_lo), y: 4, z: 8, core: 2. Of those that a mesh axis runs over, the one named last changes fastest.
Arguments:
- query_rows: bfloat16 [6144, 2048], P('seq', 'head'), may hold values from -6 to 6
- key_rows: bfloat16 [6144, 2048], P('seq', 'head'), may hold values from -6 to 6
- value_rows: bfloat16 [6144, 2048], P('seq', 'head'), may hold values from -6 to 6
- grad_output: bfloat16 [6144, 2048], P('seq', 'head'), may hold values from -6 to 6
- positions: int32 [6144], P('seq'), may hold values from 0 to 6143, each once
Outputs:
- grad_query: bfloat16 [6144, 2048], P(('seq', 'head'))
- grad_keys: bfloat16 [6144, 2048], P('seq', 'head')
- grad_values: bfloat16 [6144, 2048], P('seq', 'head')
The draws below stay inside these ranges and needn't reach their ends.
Inputs may be any that keep to these rules, and one draw needn't show every extreme that they name: `positions`: each number from 0 to 6143 appears once.
All inputs are finite; a program needn't handle non-finite values.
Results may differ from the reference program's by a relative error of at most 0.012.
Values may be sent and summed in bfloat16 or wider, within the bound.
A program may use at most 128 MiB of HBM per device.

```python
import jax
import jax.numpy as jnp
from jax import lax

HEADS = 16
HEAD_DIM = 128
TOKENS = 6144


def base_rows(key, salt):
    noise_key = jax.random.fold_in(jax.random.fold_in(key, salt), 0)
    drawn = jax.random.normal(noise_key, (TOKENS, HEADS * HEAD_DIM), jnp.float32)
    return jnp.clip(drawn, -6.0, 6.0)


def draw_query_rows(key, part):
    drawn = base_rows(key, 1)
    return drawn.astype(jnp.bfloat16)


def draw_key_rows(key, part):
    drawn = base_rows(key, 2)
    return drawn.astype(jnp.bfloat16)


def block_levels(rng, shape, shards, smallest, high):
    def one(position, parts):
        heights = jax.random.uniform(jax.random.fold_in(jax.random.fold_in(rng, 6), position), (parts,), jnp.float32, smallest / len(shards), high / len(shards))
        return jnp.repeat(jnp.exp(heights), shape[position] // parts).reshape((-1,) + (1,) * (len(shape) - position - 1))

    factor_of = one(*shards[0])
    for cut in shards[1:]:
        factor_of = factor_of * one(*cut)
    return factor_of


def scatter_about(rng, extent, spread, most, cuts=(), held_as=jnp.bfloat16):
    entries = jax.random.normal(rng, extent, jnp.float32) * spread
    if len(cuts) > 0:
        entries = block_levels(rng, extent, cuts, -0.22, 0.18) * entries
    return jnp.clip(entries, min=-most, max=most).astype(held_as)


def setup_inputs(seed: int = 0) -> dict:
    streams_of = jax.random.split(jax.random.key(seed), 6)
    return {
        "query_rows": draw_query_rows(jax.random.fold_in(streams_of[5], 71), 0),
        "key_rows": draw_key_rows(jax.random.fold_in(streams_of[5], 71), 0),
        "value_rows": scatter_about(streams_of[2], (TOKENS, HEADS * HEAD_DIM), 1.0, 6.0, ((0, 32), (1, 8))),
        "grad_output": scatter_about(streams_of[3], (TOKENS, HEADS * HEAD_DIM), 1.0, 6.0, ((0, 32), (1, 8))),
        "positions": jax.random.permutation(streams_of[4], TOKENS).astype(jnp.int32),
    }


def reference(query_rows, key_rows, value_rows, grad_output, positions):
    tokens = query_rows.shape[0]
    scaling = HEAD_DIM ** -0.5
    allowed = positions[None, :] <= positions[:, None]

    def per_head(matrix):
        return jnp.swapaxes(matrix.reshape(tokens, HEADS, HEAD_DIM), 0, 1)

    def back_rows(matrix):
        return jnp.swapaxes(matrix, 0, 1).reshape(tokens, HEADS * HEAD_DIM)

    def one_head(head_items):
        query_full = head_items[0].astype(jnp.float32)
        key_full = head_items[1].astype(jnp.float32)
        value_full = head_items[2].astype(jnp.float32)
        grad_full = head_items[3].astype(jnp.float32)
        highest = lax.Precision.HIGHEST
        scores = jnp.dot(query_full, key_full.T, precision=highest) * scaling
        masked = jnp.where(allowed, scores, -1.0e30)
        top_score = jnp.max(masked, axis=1)
        denominator = jnp.sum(jnp.where(allowed, jnp.exp(masked - top_score[:, None]), 0.0), axis=1)
        log_total = top_score + jnp.log(denominator)
        probabilities = jnp.where(allowed, jnp.exp(masked - log_total[:, None]), 0.0)
        weights = probabilities.astype(jnp.bfloat16).astype(jnp.float32)
        grad_probs = jnp.dot(grad_full, value_full.T, precision=highest)
        row_delta = jnp.sum(probabilities * grad_probs, axis=1)
        grad_value = jnp.dot(weights.T, grad_full, precision=highest)
        grad_scores = (probabilities * (grad_probs - row_delta[:, None]) * scaling).astype(jnp.bfloat16).astype(jnp.float32)
        grad_query = jnp.dot(grad_scores, key_full, precision=highest)
        grad_key = jnp.dot(grad_scores.T, query_full, precision=highest)
        return grad_query.astype(jnp.bfloat16), grad_key.astype(jnp.bfloat16), grad_value.astype(jnp.bfloat16)

    grad_query, grad_keys, grad_values = lax.map(one_head, (per_head(query_rows), per_head(key_rows), per_head(value_rows), per_head(grad_output)))
    return back_rows(grad_query), back_rows(grad_keys), back_rows(grad_values)
```

```python
import math

import jax
import jax.numpy as jnp
from jax import lax
from jax.experimental import pallas as pl
from jax.experimental.pallas import tpu as pltpu
from jax.sharding import PartitionSpec as P

MESH = pl.DeviceIdType.MESH
HEAD_DIM = 128
SCALE = HEAD_DIM**-0.5
SCALE2 = SCALE * math.log2(math.e)
FAR = -1e30
Z = 8
HOPS = 7
F32, BF16 = jnp.float32, jnp.bfloat16
NT = (((1,), (1,)), ((), ()))
TN = (((0,), (0,)), ((), ()))


def kernel(
    q_ref, k_ref, v_ref, g_ref, pos_ref, dq_ref, dk_ref, dv_ref,
    kvg, xkv, xq, qd, qf, gf, st, dpt, qpos, mx, tot, dsum, dqt,
    sibs, sibr, part, snd, rcv, xs, xr, dqs, dqr,
    in_recv, z_send, sib_send, x_send, q_recv, g_send, g_recv,
    r_send, r_recv, xr_send, xr_recv, d_send, d_recv,
):
    rows = q_ref.shape[0]
    me, hd = lax.axis_index("seq"), lax.axis_index("head")
    heads = lax.axis_size("head")
    x, z, c = lax.div(me, 16), lax.div(lax.rem(me, 16), 2), lax.rem(me, 2)

    def dev(xx, zz, cc):
        return xx * 16 + zz * 2 + cc

    up, down = dev(x, lax.rem(z + 1, Z), c), dev(x, lax.rem(z + Z - 1, Z), c)
    sibling, across = dev(x, z, 1 - c), dev(1 - x, z, c)

    def push(src, dst, send, recv, seq, head=hd):
        return pltpu.make_async_remote_copy(
            src_ref=src, dst_ref=dst, send_sem=send, recv_sem=recv,
            device_id={"seq": seq, "head": head}, device_id_type=MESH,
        )

    mine, other = pl.multiple_of(x * 128, 128), pl.multiple_of((1 - x) * 128, 128)
    kvg[me, 0:rows] = k_ref[:, pl.ds(mine, 128)]
    kvg[me, rows : 2 * rows] = v_ref[:, pl.ds(mine, 128)]
    kvg[me, 2 * rows : 2 * rows + 16] = pos_ref[...]
    xkv[0:rows] = k_ref[:, pl.ds(other, 128)]
    xkv[rows : 2 * rows] = v_ref[:, pl.ds(other, 128)]
    xkv[2 * rows : 2 * rows + 16] = pos_ref[...]
    qd[x, 0] = q_ref[:, pl.ds(mine, 128)]
    qd[x, 1] = g_ref[:, pl.ds(mine, 128)]
    xq[0] = q_ref[:, pl.ds(other, 128)]
    xq[1] = g_ref[:, pl.ds(other, 128)]

    flat = x * heads + hd

    def peer(r):
        there = lax.rem(flat + r, 2 * heads)
        return lax.div(there, heads), lax.rem(there, heads)

    barrier = pltpu.get_barrier_semaphore()
    for seq in (up, down, sibling):
        pl.semaphore_signal(barrier, inc=1, device_id={"seq": seq, "head": hd}, device_id_type=MESH)
    for r in range(1, 2 * heads):
        xx, gg = peer(r)
        pl.semaphore_signal(barrier, inc=1, device_id={"seq": dev(xx, z, c), "head": gg}, device_id_type=MESH)
    pl.semaphore_wait(barrier, 3 + 2 * heads - 1)

    def z_copy(way, s):
        return push(kvg.at[s], kvg.at[s], z_send.at[way, s], in_recv.at[s], up if way == 0 else down)

    def sib_copy(s):
        return push(kvg.at[s], kvg.at[s], sib_send.at[s], in_recv.at[s], sibling)

    partner = dev(1 - x, z, c)
    x_copy = push(xkv, kvg.at[me], x_send.at[0], in_recv.at[me], across)
    q_copy = push(xq, qd.at[x], x_send.at[1], q_recv, across)
    z_copy(0, me).start()
    z_copy(1, me).start()
    x_copy.start()
    sib_copy(me).start()
    q_copy.start()

    def arrive(s):
        sib_copy(s).wait_recv()

    mx[...] = jnp.full(mx.shape, FAR, F32)
    tot[...] = jnp.zeros(tot.shape, F32)
    dsum[...] = jnp.zeros(dsum.shape, F32)
    dqt[...] = jnp.zeros(dqt.shape, F32)

    def key_positions(s):
        block = kvg[s, 2 * rows : 2 * rows + 16].astype(F32)
        first = block[0:1] * 64.0 + block[2:3]
        rest = block[1:2] * 64.0 + block[3:4]
        columns = jnp.concatenate(
            [jnp.broadcast_to(first, (128, 128)).T, jnp.broadcast_to(rest, (128, 128)).T[0 : rows - 128]], axis=0
        )
        return columns

    def scores(s):
        raw = lax.dot_general(kvg[s, 0:rows], qf[...], NT, preferred_element_type=F32)
        grad_probs = lax.dot_general(kvg[s, rows : 2 * rows], gf[...], NT, preferred_element_type=F32)
        columns = key_positions(s)
        columns = jnp.concatenate([columns] * (2 * rows // 128), axis=1)
        raw = jnp.where(columns <= qpos[0:1], raw, FAR)
        st[s] = raw
        dpt[s] = grad_probs
        before = mx[0:1]
        top = jnp.maximum(before, jnp.max(raw, axis=0, keepdims=True))
        fade = jnp.exp2((before - top) * SCALE2)
        p = jnp.exp2((raw - top) * SCALE2)
        mx[0:1] = top
        tot[0:1] = tot[0:1] * fade + jnp.sum(p, axis=0, keepdims=True)
        dsum[0:1] = dsum[0:1] * fade + jnp.sum(p * grad_probs, axis=0, keepdims=True)

    arrive(partner)
    z_copy(0, partner).start()
    z_copy(1, partner).start()
    sib_copy(partner).start()
    q_copy.wait_recv()
    for xx in range(2):
        qf[xx * rows : (xx + 1) * rows] = qd[xx, 0]
        gf[xx * rows : (xx + 1) * rows] = qd[xx, 1]
    both = jnp.concatenate([key_positions(dev(0, z, c)), key_positions(dev(1, z, c))], axis=0)
    qpos[...] = both.T[0:8]

    def sub_of(way, e):
        far = lax.div(e, 2) + 1
        kind = lax.rem(e, 2) if way == 0 else jnp.where(e < 6, lax.rem(e, 2), 1)
        xx = x + kind - 2 * x * kind
        zz = lax.rem(z + Z - far, Z) if way == 0 else lax.rem(z + far, Z)
        return xx, zz

    def gather_step(e, carry):
        for way in range(2):
            xx, zz = sub_of(way, e)
            s = dev(xx, zz, c)
            arrive(s)
            onward = e <= 4 if way == 0 else jnp.logical_or(e <= 3, e == 5)

            @pl.when(onward)
            def _():
                z_copy(way, s).start()

            sib_copy(s).start()

        @pl.when(e == 0)
        def _():
            scores(me)
            scores(partner)

        for way in range(2):
            xx, zz = sub_of(way, e)
            scores(dev(xx, zz, c))
        for way in range(2):
            xx, zz = sub_of(way, jnp.maximum(e - 1, 0))
            first = e == 0
            xx = jnp.where(first, way, xx)
            zz = jnp.where(first, z, zz)
            s = dev(xx, zz, 1 - c)
            arrive(s)
            scores(s)
        return carry

    lax.fori_loop(0, HOPS, gather_step, 0)
    for way in range(2):
        xx, zz = sub_of(way, jnp.int32(HOPS - 1))
        s = dev(xx, zz, 1 - c)
        arrive(s)
        scores(s)

    total = tot[0:1]
    mx[0:1] = mx[0:1] * SCALE2 + jnp.log2(total)
    dsum[0:1] = dsum[0:1] / total

    def grads(s):
        p = jnp.exp2(st[s] * SCALE2 - mx[0:1])
        grad_scores = (p * (dpt[s] - dsum[0:1])).astype(BF16)
        dv = jnp.dot(p.astype(BF16), gf[...], preferred_element_type=F32)
        dk = jnp.dot(grad_scores, qf[...], preferred_element_type=F32) * SCALE
        dqt[...] += lax.dot_general(kvg[s, 0:rows], grad_scores, TN, preferred_element_type=F32)
        return dk, dv

    def g_copy(n):
        return push(sibs.at[n], sibr.at[n], g_send.at[n], g_recv.at[n], sibling)

    def r_copy(way, i):
        return push(snd.at[way, i], rcv.at[way, i], r_send.at[way, i], r_recv.at[way, i], up if way == 0 else down)

    def goal(way, i):
        far = 4 - lax.div(i + 1, 2)
        kind = lax.rem(i, 2) if way == 0 else 1 - lax.rem(i, 2)
        xx = x + kind - 2 * x * kind
        zz = lax.rem(z + far, Z) if way == 0 else lax.rem(z + Z - far, Z)
        return xx, zz

    def reduce_step(i, carry):
        for way in range(2):
            xx, zz = goal(way, i)
            dk, dv = grads(dev(xx, zz, 1 - c))
            n = 2 * i + way
            sibs[n, :, 0:128] = dk.astype(BF16)
            sibs[n, :, 128:256] = dv.astype(BF16)
            g_copy(n).start()
        for way in range(2):
            xx, zz = goal(way, i)
            dk, dv = grads(dev(xx, zz, c))
            part[way, :, 0:128] = dk
            part[way, :, 128:256] = dv
        for way in range(2):
            n = 2 * i + way
            g_copy(n).wait_recv()
            part[way] = part[way] + sibr[n].astype(F32)

            @pl.when(jnp.logical_and(i >= 2, i < HOPS))
            def _():
                r_copy(way, i - 2).wait_recv()
                part[way] = part[way] + rcv[way, i - 2].astype(F32)

            @pl.when(i < HOPS)
            def _():
                snd[way, i] = part[way].astype(BF16)
                r_copy(way, i).start()

        return carry

    lax.fori_loop(0, HOPS + 1, reduce_step, 0)

    grad_query = dqt[...].T * SCALE
    few = rows // heads
    for n in range(2 * heads):
        dqs[n] = grad_query[n * few : (n + 1) * few].astype(BF16)
    column = hd * 2 + x

    def d_copy(r):
        xx, gg = peer(r)
        n = xx * heads + gg
        return push(dqs.at[n], dqr.at[column], d_send.at[n], d_recv.at[column], dev(xx, z, c), gg)

    def d_wait(r):
        xx, gg = peer(r)
        source = gg * 2 + xx
        return push(dqs.at[0], dqr.at[source], d_send.at[0], d_recv.at[source], dev(xx, z, c), gg)

    for r in range(1, 2 * heads):
        d_copy(r).start()
    dqr[column] = dqs[flat]

    r_copy(0, 5).wait_recv()
    r_copy(1, 6).wait_recv()
    xs[...] = (part[0] + rcv[0, 5].astype(F32) + rcv[1, 6].astype(F32)).astype(BF16)
    xr_copy = push(xs, xr, xr_send, xr_recv, across)
    xr_copy.start()
    r_copy(0, 6).wait_recv()
    r_copy(1, 5).wait_recv()
    own = (part[1] + rcv[0, 6].astype(F32) + rcv[1, 5].astype(F32)).astype(BF16)
    dk_ref[:, pl.ds(mine, 128)] = own[:, 0:128]
    dv_ref[:, pl.ds(mine, 128)] = own[:, 128:256]

    for r in range(1, 2 * heads):
        d_wait(r).wait_recv()
    for n in range(2 * heads):
        dq_ref[:, n * 128 : (n + 1) * 128] = dqr[n]
    xr_copy.wait_recv()
    dk_ref[:, pl.ds(other, 128)] = xr[:, 0:128]
    dv_ref[:, pl.ds(other, 128)] = xr[:, 128:256]

    x_copy.wait_send()
    q_copy.wait_send()
    xr_copy.wait_send()
    for way in range(2):
        z_copy(way, me).wait_send()
        z_copy(way, partner).wait_send()
    sib_copy(me).wait_send()
    sib_copy(partner).wait_send()

    def drain_gather(e, carry):
        for way in range(2):
            xx, zz = sub_of(way, e)
            s = dev(xx, zz, c)
            onward = e <= 4 if way == 0 else jnp.logical_or(e <= 3, e == 5)

            @pl.when(onward)
            def _():
                z_copy(way, s).wait_send()

            sib_copy(s).wait_send()
            r_copy(way, e).wait_send()
        return carry

    lax.fori_loop(0, HOPS, drain_gather, 0)

    def drain_sums(n, carry):
        g_copy(n).wait_send()
        return carry

    lax.fori_loop(0, 2 * HOPS + 2, drain_sums, 0)
    for r in range(1, 2 * heads):
        d_copy(r).wait_send()


def local(query_rows, key_rows, value_rows, grad_output, positions):
    rows, width = query_rows.shape
    heads = lax.axis_size("head")
    members = lax.axis_size("seq")
    padded = jnp.pad(positions, (0, 256 - rows))
    coded = jnp.concatenate([padded // 64, padded % 64]).astype(BF16).reshape(4, 128)
    coded = jnp.pad(coded, ((0, 12), (0, 0)))
    vmem = pl.BlockSpec(memory_space=pltpu.VMEM)
    dma, tall = pltpu.SemaphoreType.DMA, 2 * rows + 16
    few = rows // heads
    return pl.pallas_call(
        kernel,
        out_shape=(
            jax.ShapeDtypeStruct((few, heads * width), BF16),
            jax.ShapeDtypeStruct((rows, width), BF16),
            jax.ShapeDtypeStruct((rows, width), BF16),
        ),
        in_specs=[vmem] * 5,
        out_specs=(vmem,) * 3,
        scratch_shapes=[
            pltpu.VMEM((members, tall, 128), BF16),
            pltpu.VMEM((tall, 128), BF16),
            pltpu.VMEM((2, rows, 128), BF16),
            pltpu.VMEM((2, 2, rows, 128), BF16),
            pltpu.VMEM((2 * rows, 128), BF16),
            pltpu.VMEM((2 * rows, 128), BF16),
            pltpu.VMEM((members, rows, 2 * rows), F32),
            pltpu.VMEM((members, rows, 2 * rows), F32),
            pltpu.VMEM((8, 2 * rows), F32),
            pltpu.VMEM((8, 2 * rows), F32),
            pltpu.VMEM((8, 2 * rows), F32),
            pltpu.VMEM((8, 2 * rows), F32),
            pltpu.VMEM((128, 2 * rows), F32),
            pltpu.VMEM((16, rows, 256), BF16),
            pltpu.VMEM((16, rows, 256), BF16),
            pltpu.VMEM((2, rows, 256), F32),
            pltpu.VMEM((2, HOPS, rows, 256), BF16),
            pltpu.VMEM((2, HOPS, rows, 256), BF16),
            pltpu.VMEM((rows, 256), BF16),
            pltpu.VMEM((rows, 256), BF16),
            pltpu.VMEM((2 * heads, few, 128), BF16),
            pltpu.VMEM((2 * heads, few, 128), BF16),
            dma((members,)),
            dma((2, members)),
            dma((members,)),
            dma((2,)),
            dma,
            dma((16,)),
            dma((16,)),
            dma((2, HOPS)),
            dma((2, HOPS)),
            dma,
            dma,
            dma((2 * heads,)),
            dma((2 * heads,)),
        ],
        compiler_params=pltpu.CompilerParams(
            collective_id=0, has_side_effects=True, vmem_limit_bytes=60 * 1024 * 1024
        ),
    )(query_rows, key_rows, value_rows, grad_output, coded)


def solution(mesh):
    placed = (P("seq", "head"), P("seq", "head"), P("seq", "head"), P("seq", "head"), P("seq"))
    return jax.shard_map(
        local,
        mesh=mesh,
        in_specs=placed,
        out_specs=(P(("seq", "head"), None), P("seq", "head"), P("seq", "head")),
        check_vma=False,
    )
```

```python
import math

import jax
import jax.numpy as jnp
from jax import lax
from jax.experimental import pallas as pl
from jax.experimental.pallas import tpu as pltpu
from jax.sharding import PartitionSpec as P

MESH = pl.DeviceIdType.MESH
HEAD_DIM = 128
SCALE = HEAD_DIM**-0.5
SCALE2 = SCALE * math.log2(math.e)
FAR = -1e30
Z = 8
F32, BF16 = jnp.float32, jnp.bfloat16
NT = (((1,), (1,)), ((), ()))
TN = (((0,), (0,)), ((), ()))


def kernel(
    q_ref, k_ref, v_ref, g_ref, pos_ref, dq_ref, dk_ref, dv_ref,
    kvg, xkv, xq, qf, gf, posr, posb, st, dpt, qpos, mx, tot, dsum, dqt,
    sibs, sibr, part, snd, rcv, xs, xr, dqs, dqr,
    l_sem, in_recv, z_send, sib_send, x_send, q_recv, g_send, g_recv,
    r_send, r_recv, xr_send, xr_recv, d_send, d_recv,
):
    rows = q_ref.shape[0]
    me, hd = lax.axis_index("seq"), lax.axis_index("head")
    heads = lax.axis_size("head")
    x, z, c = lax.div(me, 16), lax.div(lax.rem(me, 16), 2), lax.rem(me, 2)

    def dev(xx, zz, cc):
        return xx * 16 + zz * 2 + cc

    up, down = dev(x, lax.rem(z + 1, Z), c), dev(x, lax.rem(z + Z - 1, Z), c)
    sibling, across = dev(x, z, 1 - c), dev(1 - x, z, c)
    partner = across

    def push(src, dst, send, recv, seq, head=hd):
        return pltpu.make_async_remote_copy(
            src_ref=src, dst_ref=dst, send_sem=send, recv_sem=recv,
            device_id={"seq": seq, "head": head}, device_id_type=MESH,
        )

    vals, keys, tail = pl.ds(0, rows), pl.ds(rows, rows), pl.ds(2 * rows, 16)
    cut = (pl.ds(0, rows), pl.ds(rows, rows + 16))

    mine, other = pl.multiple_of(x * 128, 128), pl.multiple_of((1 - x) * 128, 128)
    held = pl.ds(pl.multiple_of(x * rows, rows), rows)
    loads = [
        pltpu.make_async_copy(src, dst, l_sem.at[n])
        for n, (src, dst) in enumerate((
            (pos_ref, posr),
            (v_ref.at[:, pl.ds(mine, 128)], kvg.at[me, vals]),
            (v_ref.at[:, pl.ds(other, 128)], xkv.at[vals]),
            (k_ref.at[:, pl.ds(mine, 128)], kvg.at[me, keys]),
            (k_ref.at[:, pl.ds(other, 128)], xkv.at[keys]),
            (q_ref.at[:, pl.ds(other, 128)], xq.at[0]),
            (g_ref.at[:, pl.ds(other, 128)], xq.at[1]),
            (q_ref.at[:, pl.ds(mine, 128)], qf.at[held]),
            (g_ref.at[:, pl.ds(mine, 128)], gf.at[held]),
        ))
    ]
    for load in loads:
        load.start()

    flat = x * heads + hd

    def peer(r):
        there = lax.rem(flat + r, 2 * heads)
        return lax.div(there, heads), lax.rem(there, heads)

    barrier = pltpu.get_barrier_semaphore()
    for seq in (up, down, sibling):
        pl.semaphore_signal(barrier, inc=1, device_id={"seq": seq, "head": hd}, device_id_type=MESH)
    for r in range(1, 2 * heads):
        xx, gg = peer(r)
        pl.semaphore_signal(barrier, inc=1, device_id={"seq": dev(xx, z, c), "head": gg}, device_id_type=MESH)

    mx[...] = jnp.full(mx.shape, FAR, F32)
    tot[...] = jnp.zeros(tot.shape, F32)
    dsum[...] = jnp.zeros(dsum.shape, F32)
    dqt[...] = jnp.zeros(dqt.shape, F32)

    loads[0].wait()
    place = posr[...].astype(F32)
    high = jnp.floor(place * (1.0 / 64.0))
    low = place - 64.0 * high
    posb[...] = jnp.zeros(posb.shape, F32)
    for n, digit in enumerate((high, low)):
        posb[2 * n : 2 * n + 1, :] = digit[:, 0:128]
        posb[2 * n + 1 : 2 * n + 2, 0 : rows - 128] = digit[:, 128:rows]
    kvg[me, tail] = posb[...].astype(BF16)
    xkv[tail] = posb[...].astype(BF16)

    pl.semaphore_wait(barrier, 3 + 2 * heads - 1)

    def z_copy(way, s, n, p):
        return push(kvg.at[s, cut[p]], kvg.at[s, cut[p]], z_send.at[way, n, p], in_recv.at[s, p], (up, down)[way])

    def sib_copy(s, n, p):
        return push(kvg.at[s, cut[p]], kvg.at[s, cut[p]], sib_send.at[n, p], in_recv.at[s, p], sibling)

    def x_copy(p):
        return push(xkv.at[cut[p]], kvg.at[me, cut[p]], x_send.at[p], in_recv.at[me, p], across)

    def q_copy(n):
        return push(xq.at[n], (qf, gf)[n].at[held], x_send.at[2 + n], q_recv.at[n], across)

    for p in range(2):
        loads[1 + 2 * p].wait()
        z_copy(0, me, 0, p).start()
        z_copy(1, me, 0, p).start()
        loads[2 + 2 * p].wait()
        x_copy(p).start()
        sib_copy(me, 0, p).start()
    for n in range(2):
        loads[5 + n].wait()
        q_copy(n).start()

    def arrive(s, p):
        sib_copy(s, 0, p).wait_recv()

    def key_positions(s):
        block = kvg[s, 2 * rows : 2 * rows + 16].astype(F32)
        first = block[0:1] * 64.0 + block[2:3]
        rest = block[1:2] * 64.0 + block[3:4]
        return jnp.concatenate(
            [jnp.broadcast_to(first, (128, 128)).T, jnp.broadcast_to(rest, (128, 128)).T[0 : rows - 128]], axis=0
        )

    def scores(s):
        raw = lax.dot_general(kvg[s, keys], qf[...], NT, preferred_element_type=F32)
        grad_probs = lax.dot_general(kvg[s, vals], gf[...], NT, preferred_element_type=F32)
        columns = key_positions(s)
        columns = jnp.concatenate([columns] * (2 * rows // 128), axis=1)
        raw = jnp.where(columns <= qpos[0:1], raw, FAR)
        st[s] = raw
        dpt[s] = grad_probs
        before = mx[0:1]
        top = jnp.maximum(before, jnp.max(raw, axis=0, keepdims=True))
        fade = jnp.exp2((before - top) * SCALE2)
        p = jnp.exp2((raw - top) * SCALE2)
        mx[0:1] = top
        tot[0:1] = tot[0:1] * fade + jnp.sum(p, axis=0, keepdims=True)
        dsum[0:1] = dsum[0:1] * fade + jnp.sum(p * grad_probs, axis=0, keepdims=True)

    def side(kind):
        return x + kind - 2 * x * kind

    def at(way, far):
        return lax.rem(z + Z - far, Z) if way == 0 else lax.rem(z + far, Z)

    def sib_number(way, e):
        return 2 + 6 * way + e

    def pass_on(e):
        far, kind = lax.div(e, 2) + 1, lax.rem(e, 2)
        for p in range(2):
            for way in range(2):
                s = dev(side(kind), at(way, far), c)
                arrive(s, p)
                if way + p == 1:
                    z_copy(way, s, e + 2, p).start()
                else:

                    @pl.when(far <= 2)
                    def _():
                        z_copy(way, s, e + 2, p).start()

                sib_copy(s, sib_number(way, e), p).start()

    def score_own(e):
        far, kind = lax.div(e, 2) + 1, lax.rem(e, 2)
        for way in range(2):
            scores(dev(side(kind), at(way, far), c))

    def score_sibling(e):
        far, kind = lax.div(e, 2) + 1, lax.rem(e, 2)
        for way in range(2):
            s = dev(side(kind), at(way, far), 1 - c)
            arrive(s, 0)
            arrive(s, 1)
            scores(s)

    for p in range(2):
        arrive(partner, p)
        z_copy(0, partner, 1, p).start()
        z_copy(1, partner, 1, p).start()
        sib_copy(partner, 1, p).start()
    pass_on(jnp.int32(0))
    for n in range(2):
        loads[7 + n].wait()
        q_copy(n).wait_recv()
    both = jnp.concatenate([key_positions(dev(0, z, c)), key_positions(dev(1, z, c))], axis=0)
    qpos[...] = both.T[0:8]

    def near(kind, carry):
        scores(dev(kind, z, c))
        return carry

    def near_sibling(kind, carry):
        s = dev(side(kind), z, 1 - c)
        arrive(s, 0)
        arrive(s, 1)
        scores(s)
        return carry

    lax.fori_loop(0, 2, near, 0)
    lax.fori_loop(0, 2, near_sibling, 0)

    def gather_step(e, carry):
        pass_on(e)
        score_own(e - 1)
        score_sibling(e - 1)
        return carry

    lax.fori_loop(1, 6, gather_step, 0)

    def far_pass(kind):
        for p in (1, 0):
            s = dev(side(kind), at(0, 4), c)
            arrive(s, p)
            sib_copy(s, 14 + kind, p).start()

    def far_own(kind, carry):
        scores(dev(side(kind), at(0, 4), c))
        return carry

    def far_sibling(kind, carry):
        s = dev(side(kind), at(0, 4), 1 - c)
        arrive(s, 0)
        arrive(s, 1)
        scores(s)
        return carry

    far_pass(0)
    score_own(jnp.int32(5))
    score_sibling(jnp.int32(5))
    far_pass(1)
    lax.fori_loop(0, 2, far_own, 0)
    lax.fori_loop(0, 2, far_sibling, 0)

    total = tot[0:1]
    mx[0:1] = mx[0:1] * SCALE2 + jnp.log2(total)
    dsum[0:1] = dsum[0:1] / total

    def grads(s):
        p = jnp.exp2(st[s] * SCALE2 - mx[0:1])
        grad_scores = (p * (dpt[s] - dsum[0:1])).astype(BF16)
        dv = jnp.dot(p.astype(BF16), gf[...], preferred_element_type=F32)
        dk = jnp.dot(grad_scores, qf[...], preferred_element_type=F32) * SCALE
        dqt[...] += lax.dot_general(kvg[s, keys], grad_scores, TN, preferred_element_type=F32)
        return dv, dk

    def g_copy(n):
        return push(sibs.at[n], sibr.at[n], g_send.at[n], g_recv.at[n], sibling)

    def r_copy(way, h, p):
        return push(snd.at[way, h, p], rcv.at[way, h, p], r_send.at[way, h, p], r_recv.at[way, h, p], (up, down)[way])

    def for_sibling(s, n):
        for p, term in enumerate(grads(s)):
            sibs[n, p] = term.astype(BF16)
        g_copy(n).start()

    def for_own(s, way):
        for p, term in enumerate(grads(s)):
            part[way, p] = term

    def farthest(h, carry):
        s = side(1 - h)
        for_sibling(dev(s, at(1, 4), 1 - c), h)
        for_own(dev(s, at(1, 4), c), 0)
        g_copy(h).wait_recv()
        for way in range(2):
            p = 1 - way
            snd[way, h, p] = (part[0, p] + sibr[h, p].astype(F32)).astype(BF16)
            r_copy(way, h, p).start()
        return carry

    lax.fori_loop(0, 2, farthest, 0)

    def reduce_step(h, carry):
        far = 4 - lax.div(h, 2)
        xx = side(1 - lax.rem(h, 2))
        n = 2 * h - 2
        for way in range(2):
            for_sibling(dev(xx, at(1 - way, far), 1 - c), n + way)
        for way in range(2):
            for_own(dev(xx, at(1 - way, far), c), way)
        for way in range(2):
            g_copy(n + way).wait_recv()
        for turn in range(2):
            for way in range(2):
                p = turn if way == 0 else 1 - turn
                here = part[way, p] + sibr[n + way, p].astype(F32)
                if turn == 0:

                    @pl.when(h >= 4)
                    def _():
                        r_copy(way, h - 2, p).wait_recv()
                        snd[way, h, p] = (here + rcv[way, h - 2, p].astype(F32)).astype(BF16)

                    @pl.when(h < 4)
                    def _():
                        snd[way, h, p] = here.astype(BF16)

                else:
                    r_copy(way, h - 2, p).wait_recv()
                    snd[way, h, p] = (here + rcv[way, h - 2, p].astype(F32)).astype(BF16)
                r_copy(way, h, p).start()
        return carry

    lax.fori_loop(2, 8, reduce_step, 0)

    def home_sibling(h, carry):
        for_sibling(dev(side(1 - h), z, 1 - c), 14 + h)
        return carry

    def home(h, carry):
        for_own(dev(side(1 - h), z, c), h)
        return carry

    lax.fori_loop(0, 2, home_sibling, 0)
    lax.fori_loop(0, 2, home, 0)

    grad_query = dqt[...].T * SCALE
    few = rows // heads
    for n in range(2 * heads):
        dqs[n] = grad_query[n * few : (n + 1) * few].astype(BF16)
    column = hd * 2 + x

    def d_copy(r):
        xx, gg = peer(r)
        n = xx * heads + gg
        return push(dqs.at[n], dqr.at[column], d_send.at[n], d_recv.at[column], dev(xx, z, c), gg)

    def d_wait(r):
        xx, gg = peer(r)
        source = gg * 2 + xx
        return push(dqs.at[0], dqr.at[source], d_send.at[0], d_recv.at[source], dev(xx, z, c), gg)

    for r in range(1, 2 * heads):
        d_copy(r).start()
    dqr[column] = dqs[flat]
    for h in range(2):
        g_copy(14 + h).wait_recv()

    def final(h, p):
        for way in range(2):
            r_copy(way, 6 + h, p).wait_recv()
        terms = part[h, p] + sibr[14 + h, p].astype(F32)
        return (terms + rcv[0, 6 + h, p].astype(F32) + rcv[1, 6 + h, p].astype(F32)).astype(BF16)

    def xr_copy(p):
        return push(xs.at[p], xr.at[p], xr_send.at[p], xr_recv.at[p], across)

    outs = (dv_ref, dk_ref)
    for p in range(2):
        xs[p] = final(0, p)
        xr_copy(p).start()
    for r in range(1, 2 * heads):
        d_wait(r).wait_recv()
    for n in range(2 * heads):
        dq_ref[:, n * 128 : (n + 1) * 128] = dqr[n]
    for p in range(2):
        outs[p][:, pl.ds(mine, 128)] = final(1, p)

    for way in range(2):
        for p in range(2):
            z_copy(way, me, 0, p).wait_send()
            z_copy(way, partner, 1, p).wait_send()

    def drain_gather(e, carry):
        for p in range(2):
            for way in range(2):
                if way + p == 1:
                    z_copy(way, me, e + 2, p).wait_send()
                else:

                    @pl.when(e < 4)
                    def _():
                        z_copy(way, me, e + 2, p).wait_send()

                r_copy(way, e + 2, p).wait_send()
        return carry

    lax.fori_loop(0, 6, drain_gather, 0)

    def drain_sibling(n, carry):
        for p in range(2):
            sib_copy(me, n, p).wait_send()
        g_copy(n).wait_send()
        return carry

    lax.fori_loop(0, 16, drain_sibling, 0)
    for h in range(2):
        r_copy(0, h, 1).wait_send()
        r_copy(1, h, 0).wait_send()
        x_copy(h).wait_send()
        q_copy(h).wait_send()
    for r in range(1, 2 * heads):
        d_copy(r).wait_send()
    for p in range(2):
        xr_copy(p).wait_recv()
        outs[p][:, pl.ds(other, 128)] = xr[p]
        xr_copy(p).wait_send()


def local(query_rows, key_rows, value_rows, grad_output, positions):
    rows, width = query_rows.shape
    heads = lax.axis_size("head")
    members = lax.axis_size("seq")
    vmem = pl.BlockSpec(memory_space=pltpu.VMEM)
    dma, tall = pltpu.SemaphoreType.DMA, 2 * rows + 16
    few = rows // heads
    return pl.pallas_call(
        kernel,
        out_shape=(
            pltpu.VMEM((few, heads * width), BF16),
            pltpu.VMEM((rows, width), BF16),
            pltpu.VMEM((rows, width), BF16),
        ),
        in_specs=[pl.BlockSpec(memory_space=pl.ANY)] * 5,
        out_specs=(vmem,) * 3,
        scratch_shapes=[
            pltpu.VMEM((members, tall, 128), BF16),
            pltpu.VMEM((tall, 128), BF16),
            pltpu.VMEM((2, rows, 128), BF16),
            pltpu.VMEM((2 * rows, 128), BF16),
            pltpu.VMEM((2 * rows, 128), BF16),
            pltpu.VMEM((1, rows), jnp.int32),
            pltpu.VMEM((16, 128), F32),
            pltpu.VMEM((members, rows, 2 * rows), F32),
            pltpu.VMEM((members, rows, 2 * rows), F32),
            pltpu.VMEM((8, 2 * rows), F32),
            pltpu.VMEM((8, 2 * rows), F32),
            pltpu.VMEM((8, 2 * rows), F32),
            pltpu.VMEM((8, 2 * rows), F32),
            pltpu.VMEM((128, 2 * rows), F32),
            pltpu.VMEM((16, 2, rows, 128), BF16),
            pltpu.VMEM((16, 2, rows, 128), BF16),
            pltpu.VMEM((2, 2, rows, 128), F32),
            pltpu.VMEM((2, 8, 2, rows, 128), BF16),
            pltpu.VMEM((2, 8, 2, rows, 128), BF16),
            pltpu.VMEM((2, rows, 128), BF16),
            pltpu.VMEM((2, rows, 128), BF16),
            pltpu.VMEM((2 * heads, few, 128), BF16),
            pltpu.VMEM((2 * heads, few, 128), BF16),
            dma((9,)),
            dma((members, 2)),
            dma((2, 8, 2)),
            dma((16, 2)),
            dma((4,)),
            dma((2,)),
            dma((16,)),
            dma((16,)),
            dma((2, 8, 2)),
            dma((2, 8, 2)),
            dma((2,)),
            dma((2,)),
            dma((2 * heads,)),
            dma((2 * heads,)),
        ],
        compiler_params=pltpu.CompilerParams(
            collective_id=0, has_side_effects=True, vmem_limit_bytes=60 * 1024 * 1024
        ),
    )(query_rows, key_rows, value_rows, grad_output, positions.reshape(1, rows))


def solution(mesh):
    placed = (P("seq", "head"), P("seq", "head"), P("seq", "head"), P("seq", "head"), P("seq"))
    return jax.shard_map(
        local,
        mesh=mesh,
        in_specs=placed,
        out_specs=(P(("seq", "head"), None), P("seq", "head"), P("seq", "head")),
        check_vma=False,
    )
```

```python
import math

import jax
import jax.numpy as jnp
from jax import lax
from jax.experimental import pallas as pl
from jax.experimental.pallas import tpu as pltpu
from jax.sharding import PartitionSpec as P

MESH = pl.DeviceIdType.MESH
HEAD_DIM = 128
SCALE = HEAD_DIM**-0.5
SCALE2 = SCALE * math.log2(math.e)
FAR = -1e30
Z = 8
F32, BF16 = jnp.float32, jnp.bfloat16
NT = (((1,), (1,)), ((), ()))
TN = (((0,), (0,)), ((), ()))


def kernel(
    q_ref, k_ref, v_ref, g_ref, pos_ref, dq_ref, dk_ref, dv_ref,
    kvg, xkv, xq, qf, gf, posr, posb, st, dpt, qpos, mx, tot, dsum, dqt,
    sibs, sibr, part, snd, rcv, xs, xr, dqs, dqr,
    l_sem, in_recv, z_send, sib_send, x_send, q_recv, g_send, g_recv,
    r_send, r_recv, xr_send, xr_recv, d_send, d_recv, near_sem, go_sem, far_sem,
):
    rows = q_ref.shape[0]
    me, hd = lax.axis_index("seq"), lax.axis_index("head")
    heads = lax.axis_size("head")
    x, z, c = lax.div(me, 16), lax.div(lax.rem(me, 16), 2), lax.rem(me, 2)

    def dev(xx, zz, cc):
        return xx * 16 + zz * 2 + cc

    up, down = dev(x, lax.rem(z + 1, Z), c), dev(x, lax.rem(z + Z - 1, Z), c)
    sibling, across = dev(x, z, 1 - c), dev(1 - x, z, c)
    partner = across

    def push(src, dst, send, recv, seq, head=hd):
        return pltpu.make_async_remote_copy(
            src_ref=src, dst_ref=dst, send_sem=send, recv_sem=recv,
            device_id={"seq": seq, "head": head}, device_id_type=MESH,
        )

    vals, keys, tail = pl.ds(0, rows), pl.ds(rows, rows), pl.ds(2 * rows, 16)
    cut = (pl.ds(0, rows), pl.ds(rows, rows + 16))

    mine, other = pl.multiple_of(x * 128, 128), pl.multiple_of((1 - x) * 128, 128)
    held = pl.ds(pl.multiple_of(x * rows, rows), rows)
    loads = [
        pltpu.make_async_copy(src, dst, l_sem.at[n])
        for n, (src, dst) in enumerate((
            (pos_ref, posr),
            (v_ref.at[:, pl.ds(mine, 128)], kvg.at[me, vals]),
            (v_ref.at[:, pl.ds(other, 128)], xkv.at[vals]),
            (k_ref.at[:, pl.ds(mine, 128)], kvg.at[me, keys]),
            (k_ref.at[:, pl.ds(other, 128)], xkv.at[keys]),
            (q_ref.at[:, pl.ds(other, 128)], xq.at[0]),
            (g_ref.at[:, pl.ds(other, 128)], xq.at[1]),
            (q_ref.at[:, pl.ds(mine, 128)], qf.at[held]),
            (g_ref.at[:, pl.ds(mine, 128)], gf.at[held]),
        ))
    ]
    for load in loads:
        load.start()

    flat = x * heads + hd

    def peer(r):
        there = lax.rem(flat + r, 2 * heads)
        return lax.div(there, heads), lax.rem(there, heads)

    barrier = pltpu.get_barrier_semaphore()

    def signal(sem, seq, head=hd):
        pl.semaphore_signal(sem, inc=1, device_id={"seq": seq, "head": head}, device_id_type=MESH)

    @pl.when(c == 1)
    def _():
        for seq in (up, down, across):
            signal(barrier, seq)

    @pl.when(c == 0)
    def _():
        signal(barrier, sibling)

    mx[...] = jnp.full(mx.shape, FAR, F32)
    tot[...] = jnp.zeros(tot.shape, F32)
    dsum[...] = jnp.zeros(dsum.shape, F32)
    dqt[...] = jnp.zeros(dqt.shape, F32)

    loads[0].wait()
    place = posr[...].astype(F32)
    high = jnp.floor(place * (1.0 / 64.0))
    low = place - 64.0 * high
    posb[...] = jnp.zeros(posb.shape, F32)
    for n, digit in enumerate((high, low)):
        posb[2 * n : 2 * n + 1, :] = digit[:, 0:128]
        posb[2 * n + 1 : 2 * n + 2, 0 : rows - 128] = digit[:, 128:rows]
    kvg[me, tail] = posb[...].astype(BF16)
    xkv[tail] = posb[...].astype(BF16)

    @pl.when(c == 1)
    def _():
        pl.semaphore_wait(barrier, 4)
        for seq in (up, down, across):
            signal(near_sem, seq)

    @pl.when(c == 0)
    def _():
        pl.semaphore_wait(go_sem, 1)

    def z_copy(way, s, n, p):
        return push(kvg.at[s, cut[p]], kvg.at[s, cut[p]], z_send.at[way, n, p], in_recv.at[s, p], (up, down)[way])

    def sib_copy(s, n, p):
        return push(kvg.at[s, cut[p]], kvg.at[s, cut[p]], sib_send.at[n, p], in_recv.at[s, p], sibling)

    def x_copy(p):
        return push(xkv.at[cut[p]], kvg.at[me, cut[p]], x_send.at[p], in_recv.at[me, p], across)

    def q_copy(n):
        return push(xq.at[n], (qf, gf)[n].at[held], x_send.at[2 + n], q_recv.at[n], across)

    for p in range(2):
        loads[1 + 2 * p].wait()
        z_copy(0, me, 0, p).start()
        z_copy(1, me, 0, p).start()
        loads[2 + 2 * p].wait()
        x_copy(p).start()
        sib_copy(me, 0, p).start()
    for n in range(2):
        loads[5 + n].wait()
        q_copy(n).start()

    @pl.when(c == 1)
    def _():
        pl.semaphore_wait(near_sem, 3)
        signal(go_sem, sibling)

    @pl.when(c == 0)
    def _():
        for xx in range(2):
            for r in range(1, heads):
                signal(barrier, dev(xx, z, c), lax.rem(hd + r, heads))

    def arrive(s, p):
        sib_copy(s, 0, p).wait_recv()

    def key_positions(s):
        block = kvg[s, 2 * rows : 2 * rows + 16].astype(F32)
        first = block[0:1] * 64.0 + block[2:3]
        rest = block[1:2] * 64.0 + block[3:4]
        return jnp.concatenate(
            [jnp.broadcast_to(first, (128, 128)).T, jnp.broadcast_to(rest, (128, 128)).T[0 : rows - 128]], axis=0
        )

    def scores(s):
        raw = lax.dot_general(kvg[s, keys], qf[...], NT, preferred_element_type=F32)
        grad_probs = lax.dot_general(kvg[s, vals], gf[...], NT, preferred_element_type=F32)
        columns = key_positions(s)
        columns = jnp.concatenate([columns] * (2 * rows // 128), axis=1)
        raw = jnp.where(columns <= qpos[0:1], raw, FAR)
        st[s] = raw
        dpt[s] = grad_probs
        before = mx[0:1]
        top = jnp.maximum(before, jnp.max(raw, axis=0, keepdims=True))
        fade = jnp.exp2((before - top) * SCALE2)
        p = jnp.exp2((raw - top) * SCALE2)
        mx[0:1] = top
        tot[0:1] = tot[0:1] * fade + jnp.sum(p, axis=0, keepdims=True)
        dsum[0:1] = dsum[0:1] * fade + jnp.sum(p * grad_probs, axis=0, keepdims=True)

    def side(kind):
        return x + kind - 2 * x * kind

    def at(way, far):
        return lax.rem(z + Z - far, Z) if way == 0 else lax.rem(z + far, Z)

    def sib_number(way, e):
        return 2 + 6 * way + e

    def pass_on(e):
        far, kind = lax.div(e, 2) + 1, lax.rem(e, 2)
        for p in range(2):
            for way in range(2):
                s = dev(side(kind), at(way, far), c)
                arrive(s, p)
                if way + p == 1:
                    z_copy(way, s, e + 2, p).start()
                else:

                    @pl.when(far <= 2)
                    def _():
                        z_copy(way, s, e + 2, p).start()

                sib_copy(s, sib_number(way, e), p).start()

    def score_own(e):
        far, kind = lax.div(e, 2) + 1, lax.rem(e, 2)
        for way in range(2):
            scores(dev(side(kind), at(way, far), c))

    def score_sibling(e):
        far, kind = lax.div(e, 2) + 1, lax.rem(e, 2)
        for way in range(2):
            s = dev(side(kind), at(way, far), 1 - c)
            arrive(s, 0)
            arrive(s, 1)
            scores(s)

    for p in range(2):
        arrive(partner, p)
        z_copy(0, partner, 1, p).start()
        z_copy(1, partner, 1, p).start()
        sib_copy(partner, 1, p).start()
    pass_on(jnp.int32(0))
    for n in range(2):
        loads[7 + n].wait()
        q_copy(n).wait_recv()
    both = jnp.concatenate([key_positions(dev(0, z, c)), key_positions(dev(1, z, c))], axis=0)
    qpos[...] = both.T[0:8]

    def near(kind, carry):
        scores(dev(kind, z, c))
        return carry

    def near_sibling(kind, carry):
        s = dev(side(kind), z, 1 - c)
        arrive(s, 0)
        arrive(s, 1)
        scores(s)
        return carry

    lax.fori_loop(0, 2, near, 0)
    lax.fori_loop(0, 2, near_sibling, 0)

    def gather_step(e, carry):
        pass_on(e)
        score_own(e - 1)
        score_sibling(e - 1)
        return carry

    lax.fori_loop(1, 6, gather_step, 0)

    def far_pass(kind):
        for p in (1, 0):
            s = dev(side(kind), at(0, 4), c)
            arrive(s, p)
            sib_copy(s, 14 + kind, p).start()

    def far_own(kind, carry):
        scores(dev(side(kind), at(0, 4), c))
        return carry

    def far_sibling(kind, carry):
        s = dev(side(kind), at(0, 4), 1 - c)
        arrive(s, 0)
        arrive(s, 1)
        scores(s)
        return carry

    far_pass(0)
    score_own(jnp.int32(5))
    score_sibling(jnp.int32(5))
    far_pass(1)
    lax.fori_loop(0, 2, far_own, 0)
    lax.fori_loop(0, 2, far_sibling, 0)

    total = tot[0:1]
    mx[0:1] = mx[0:1] * SCALE2 + jnp.log2(total)
    dsum[0:1] = dsum[0:1] / total

    def grads(s):
        p = jnp.exp2(st[s] * SCALE2 - mx[0:1])
        grad_scores = (p * (dpt[s] - dsum[0:1])).astype(BF16)
        dv = jnp.dot(p.astype(BF16), gf[...], preferred_element_type=F32)
        dk = jnp.dot(grad_scores, qf[...], preferred_element_type=F32) * SCALE
        dqt[...] += lax.dot_general(kvg[s, keys], grad_scores, TN, preferred_element_type=F32)
        return dv, dk

    def g_copy(n):
        return push(sibs.at[n], sibr.at[n], g_send.at[n], g_recv.at[n], sibling)

    def r_copy(way, h, p):
        return push(snd.at[way, h, p], rcv.at[way, h, p], r_send.at[way, h, p], r_recv.at[way, h, p], (up, down)[way])

    def for_sibling(s, n):
        for p, term in enumerate(grads(s)):
            sibs[n, p] = term.astype(BF16)
        g_copy(n).start()

    def for_own(s, h, way):
        for p, term in enumerate(grads(s)):
            part[h, way, p] = term

    def farthest(h, carry):
        s = side(1 - h)
        for_sibling(dev(s, at(1, 4), 1 - c), h)
        for_own(dev(s, at(1, 4), c), h, 0)
        g_copy(h).wait_recv()
        for way in range(2):
            p = 1 - way
            snd[way, h, p] = (part[h, 0, p] + sibr[h, p].astype(F32)).astype(BF16)
            r_copy(way, h, p).start()
        return carry

    lax.fori_loop(0, 2, farthest, 0)

    def step_terms(h):
        far = 4 - lax.div(h, 2)
        for way in range(2):
            xx = side(jnp.where(h == 8, 1 - way, 1 - lax.rem(h, 2)))
            for_sibling(dev(xx, at(1 - way, far), 1 - c), 2 * h - 2 + way)
        for way in range(2):
            xx = side(jnp.where(h == 8, 1 - way, 1 - lax.rem(h, 2)))
            for_own(dev(xx, at(1 - way, far), c), h, way)

    def here(h, way, p):
        return part[h, way, p] + sibr[2 * h - 2 + way, p].astype(F32)

    def send_first(h):
        for way in range(2):
            g_copy(2 * h - 2 + way).wait_recv()
            snd[way, h, way] = here(h, way, way).astype(BF16)
            r_copy(way, h, way).start()

    def send_summed(h, turn):
        for way in range(2):
            p = turn if way == 0 else 1 - turn
            r_copy(way, h - 2, p).wait_recv()
            snd[way, h, p] = (here(h, way, p) + rcv[way, h - 2, p].astype(F32)).astype(BF16)
            r_copy(way, h, p).start()

    def send_both(h):
        for way in range(2):
            g_copy(2 * h - 2 + way).wait_recv()
        send_summed(h, 0)
        send_summed(h, 1)

    def first_step(h, carry):
        step_terms(h)
        send_first(h)
        return carry

    lax.fori_loop(2, 4, first_step, 0)

    def reduce_step(h, carry):
        step_terms(h)

        @pl.when(h == 4)
        def _():
            send_summed(jnp.int32(2), 1)
            send_summed(jnp.int32(3), 1)

        @pl.when(jnp.logical_and(h > 4, h < 8))
        def _():
            send_both(h - 1)

        return carry

    lax.fori_loop(4, 9, reduce_step, 0)

    grad_query = dqt[...].T * SCALE
    few = rows // heads
    for n in range(2 * heads):
        dqs[n] = grad_query[n * few : (n + 1) * few].astype(BF16)
    column = hd * 2 + x

    def d_copy(r):
        xx, gg = peer(r)
        n = xx * heads + gg
        return push(dqs.at[n], dqr.at[column], d_send.at[n], d_recv.at[column], dev(xx, z, c), gg)

    def d_wait(r):
        xx, gg = peer(r)
        source = gg * 2 + xx
        return push(dqs.at[0], dqr.at[source], d_send.at[0], d_recv.at[source], dev(xx, z, c), gg)

    @pl.when(c == 0)
    def _():
        pl.semaphore_wait(barrier, 2 * heads - 2)
        signal(far_sem, sibling)

    @pl.when(c == 1)
    def _():
        pl.semaphore_wait(far_sem, 1)

    for r in range(1, 2 * heads):
        d_copy(r).start()
    dqr[column] = dqs[flat]
    send_both(jnp.int32(7))
    for h in range(2):
        g_copy(14 + h).wait_recv()

    def final(h, p):
        for way in range(2):
            r_copy(way, 6 + h, p).wait_recv()
        terms = part[8, h, p] + sibr[14 + h, p].astype(F32)
        return (terms + rcv[0, 6 + h, p].astype(F32) + rcv[1, 6 + h, p].astype(F32)).astype(BF16)

    def xr_copy(p):
        return push(xs.at[p], xr.at[p], xr_send.at[p], xr_recv.at[p], across)

    outs = (dv_ref, dk_ref)
    for p in range(2):
        xs[p] = final(0, p)
        xr_copy(p).start()
    for p in range(2):
        outs[p][:, pl.ds(mine, 128)] = final(1, p)
    for r in range(1, 2 * heads):
        d_wait(r).wait_recv()
    for n in range(2 * heads):
        dq_ref[:, n * 128 : (n + 1) * 128] = dqr[n]

    for way in range(2):
        for p in range(2):
            z_copy(way, me, 0, p).wait_send()
            z_copy(way, partner, 1, p).wait_send()

    def drain_gather(e, carry):
        for p in range(2):
            for way in range(2):
                if way + p == 1:
                    z_copy(way, me, e + 2, p).wait_send()
                else:

                    @pl.when(e < 4)
                    def _():
                        z_copy(way, me, e + 2, p).wait_send()

                r_copy(way, e + 2, p).wait_send()
        return carry

    lax.fori_loop(0, 6, drain_gather, 0)

    def drain_sibling(n, carry):
        for p in range(2):
            sib_copy(me, n, p).wait_send()
        g_copy(n).wait_send()
        return carry

    lax.fori_loop(0, 16, drain_sibling, 0)
    for h in range(2):
        r_copy(0, h, 1).wait_send()
        r_copy(1, h, 0).wait_send()
        x_copy(h).wait_send()
        q_copy(h).wait_send()
    for r in range(1, 2 * heads):
        d_copy(r).wait_send()
    for p in range(2):
        xr_copy(p).wait_recv()
        outs[p][:, pl.ds(other, 128)] = xr[p]
        xr_copy(p).wait_send()


def local(query_rows, key_rows, value_rows, grad_output, positions):
    rows, width = query_rows.shape
    heads = lax.axis_size("head")
    members = lax.axis_size("seq")
    vmem = pl.BlockSpec(memory_space=pltpu.VMEM)
    dma, tall = pltpu.SemaphoreType.DMA, 2 * rows + 16
    few = rows // heads
    return pl.pallas_call(
        kernel,
        out_shape=(
            pltpu.VMEM((few, heads * width), BF16),
            pltpu.VMEM((rows, width), BF16),
            pltpu.VMEM((rows, width), BF16),
        ),
        in_specs=[pl.BlockSpec(memory_space=pl.ANY)] * 5,
        out_specs=(vmem,) * 3,
        scratch_shapes=[
            pltpu.VMEM((members, tall, 128), BF16),
            pltpu.VMEM((tall, 128), BF16),
            pltpu.VMEM((2, rows, 128), BF16),
            pltpu.VMEM((2 * rows, 128), BF16),
            pltpu.VMEM((2 * rows, 128), BF16),
            pltpu.VMEM((1, rows), jnp.int32),
            pltpu.VMEM((16, 128), F32),
            pltpu.VMEM((members, rows, 2 * rows), F32),
            pltpu.VMEM((members, rows, 2 * rows), F32),
            pltpu.VMEM((8, 2 * rows), F32),
            pltpu.VMEM((8, 2 * rows), F32),
            pltpu.VMEM((8, 2 * rows), F32),
            pltpu.VMEM((8, 2 * rows), F32),
            pltpu.VMEM((128, 2 * rows), F32),
            pltpu.VMEM((16, 2, rows, 128), BF16),
            pltpu.VMEM((16, 2, rows, 128), BF16),
            pltpu.VMEM((9, 2, 2, rows, 128), F32),
            pltpu.VMEM((2, 8, 2, rows, 128), BF16),
            pltpu.VMEM((2, 8, 2, rows, 128), BF16),
            pltpu.VMEM((2, rows, 128), BF16),
            pltpu.VMEM((2, rows, 128), BF16),
            pltpu.VMEM((2 * heads, few, 128), BF16),
            pltpu.VMEM((2 * heads, few, 128), BF16),
            dma((9,)),
            dma((members, 2)),
            dma((2, 8, 2)),
            dma((16, 2)),
            dma((4,)),
            dma((2,)),
            dma((16,)),
            dma((16,)),
            dma((2, 8, 2)),
            dma((2, 8, 2)),
            dma((2,)),
            dma((2,)),
            dma((2 * heads,)),
            dma((2 * heads,)),
            pltpu.SemaphoreType.REGULAR,
            pltpu.SemaphoreType.REGULAR,
            pltpu.SemaphoreType.REGULAR,
        ],
        compiler_params=pltpu.CompilerParams(
            collective_id=0, has_side_effects=True, vmem_limit_bytes=60 * 1024 * 1024
        ),
    )(query_rows, key_rows, value_rows, grad_output, positions.reshape(1, rows))


def solution(mesh):
    placed = (P("seq", "head"), P("seq", "head"), P("seq", "head"), P("seq", "head"), P("seq"))
    return jax.shard_map(
        local,
        mesh=mesh,
        in_specs=placed,
        out_specs=(P(("seq", "head"), None), P("seq", "head"), P("seq", "head")),
        check_vma=False,
    )
```

```python
import math

import jax
import jax.numpy as jnp
from jax import lax
from jax.experimental import pallas as pl
from jax.experimental.pallas import tpu as pltpu
from jax.sharding import PartitionSpec as P

MESH = pl.DeviceIdType.MESH
HEAD_DIM = 128
SCALE = HEAD_DIM**-0.5
SCALE2 = SCALE * math.log2(math.e)
FAR = -1e30
Z = 8
PIECES = 4
F32, BF16 = jnp.float32, jnp.bfloat16
NT = (((1,), (1,)), ((), ()))
TN = (((0,), (0,)), ((), ()))


def kernel(
    q_ref, k_ref, v_ref, g_ref, pos_ref, dq_ref, dk_ref, dv_ref,
    kvg, xkv, xq, qf, gf, posr, posb, st, dpt, qpos, mx, tot, dsum, dqt,
    sibs, sibr, part, snd, rcv, xs, xr, dqs, dqr,
    l_sem, in_recv, z_send, sib_send, x_send, q_recv, g_send, g_recv,
    r_send, r_recv, xr_send, xr_recv, d_send, d_recv, near_sem, go_sem, far_sem,
):
    rows = q_ref.shape[0]
    me, hd = lax.axis_index("seq"), lax.axis_index("head")
    heads = lax.axis_size("head")
    x, z, c = lax.div(me, 16), lax.div(lax.rem(me, 16), 2), lax.rem(me, 2)

    def dev(xx, zz, cc):
        return xx * 16 + zz * 2 + cc

    up, down = dev(x, lax.rem(z + 1, Z), c), dev(x, lax.rem(z + Z - 1, Z), c)
    sibling, across = dev(x, z, 1 - c), dev(1 - x, z, c)
    partner = across

    def push(src, dst, send, recv, seq, head=hd):
        return pltpu.make_async_remote_copy(
            src_ref=src, dst_ref=dst, send_sem=send, recv_sem=recv,
            device_id={"seq": seq, "head": head}, device_id_type=MESH,
        )

    vals, keys, tail = pl.ds(0, rows), pl.ds(rows, rows), pl.ds(2 * rows, 8)
    some = rows // 2
    cut = (pl.ds(0, some), pl.ds(some, some), pl.ds(rows, some), pl.ds(rows + some, some + 8))

    mine, other = pl.multiple_of(x * 128, 128), pl.multiple_of((1 - x) * 128, 128)
    held = pl.ds(pl.multiple_of(x * rows, rows), rows)
    loads = [
        pltpu.make_async_copy(src, dst, l_sem.at[n])
        for n, (src, dst) in enumerate((
            (pos_ref, posr),
            (v_ref.at[:, pl.ds(mine, 128)], kvg.at[me, vals]),
            (v_ref.at[:, pl.ds(other, 128)], xkv.at[vals]),
            (k_ref.at[:, pl.ds(mine, 128)], kvg.at[me, keys]),
            (k_ref.at[:, pl.ds(other, 128)], xkv.at[keys]),
            (q_ref.at[:, pl.ds(other, 128)], xq.at[0]),
            (g_ref.at[:, pl.ds(other, 128)], xq.at[1]),
            (q_ref.at[:, pl.ds(mine, 128)], qf.at[held]),
            (g_ref.at[:, pl.ds(mine, 128)], gf.at[held]),
        ))
    ]
    for load in loads:
        load.start()

    flat = x * heads + hd

    def peer(r):
        there = lax.rem(flat + r, 2 * heads)
        return lax.div(there, heads), lax.rem(there, heads)

    barrier = pltpu.get_barrier_semaphore()

    def signal(sem, seq, head=hd):
        pl.semaphore_signal(sem, inc=1, device_id={"seq": seq, "head": head}, device_id_type=MESH)

    @pl.when(c == 1)
    def _():
        for seq in (up, down, across):
            signal(barrier, seq)

    @pl.when(c == 0)
    def _():
        signal(barrier, sibling)

    mx[...] = jnp.full(mx.shape, FAR, F32)
    tot[...] = jnp.zeros(tot.shape, F32)
    dsum[...] = jnp.zeros(dsum.shape, F32)
    dqt[...] = jnp.zeros(dqt.shape, F32)

    loads[0].wait()
    place = posr[...].astype(F32)
    high = jnp.floor(place * (1.0 / 64.0))
    low = place - 64.0 * high
    posb[...] = jnp.zeros(posb.shape, F32)
    for n, digit in enumerate((high, low)):
        posb[2 * n : 2 * n + 1, :] = digit[:, 0:128]
        posb[2 * n + 1 : 2 * n + 2, 0 : rows - 128] = digit[:, 128:rows]
    kvg[me, tail] = posb[...].astype(BF16)
    xkv[tail] = posb[...].astype(BF16)

    @pl.when(c == 1)
    def _():
        pl.semaphore_wait(barrier, 4)
        for seq in (up, down, across):
            signal(near_sem, seq)

    @pl.when(c == 0)
    def _():
        pl.semaphore_wait(go_sem, 1)

    def z_copy(way, s, n, p):
        return push(kvg.at[s, cut[p]], kvg.at[s, cut[p]], z_send.at[way, n, p], in_recv.at[s, p], (up, down)[way])

    def sib_copy(s, n, p):
        return push(kvg.at[s, cut[p]], kvg.at[s, cut[p]], sib_send.at[n, p], in_recv.at[s, p], sibling)

    def x_copy(p):
        return push(xkv.at[cut[p]], kvg.at[me, cut[p]], x_send.at[p], in_recv.at[me, p], across)

    def q_copy(n):
        return push(xq.at[n], (qf, gf)[n].at[held], x_send.at[4 + n], q_recv.at[n], across)

    for half in range(2):
        loads[1 + 2 * half].wait()
        loads[2 + 2 * half].wait()
        for p in (2 * half, 2 * half + 1):
            z_copy(0, me, 0, p).start()
            z_copy(1, me, 0, p).start()
            x_copy(p).start()
        for p in (2 * half, 2 * half + 1):
            sib_copy(me, 0, p).start()
    for n in range(2):
        loads[5 + n].wait()
        q_copy(n).start()

    @pl.when(c == 1)
    def _():
        pl.semaphore_wait(near_sem, 3)
        signal(go_sem, sibling)

    @pl.when(c == 0)
    def _():
        for xx in range(2):
            for r in range(1, heads):
                signal(barrier, dev(xx, z, c), lax.rem(hd + r, heads))

    def arrive(s, p):
        sib_copy(s, 0, p).wait_recv()

    def key_positions(s):
        block = kvg[s, 2 * rows : 2 * rows + 8].astype(F32)
        first = block[0:1] * 64.0 + block[2:3]
        rest = block[1:2] * 64.0 + block[3:4]
        return jnp.concatenate(
            [jnp.broadcast_to(first, (128, 128)).T, jnp.broadcast_to(rest, (128, 128)).T[0 : rows - 128]], axis=0
        )

    def scores(s):
        raw = lax.dot_general(kvg[s, keys], qf[...], NT, preferred_element_type=F32)
        grad_probs = lax.dot_general(kvg[s, vals], gf[...], NT, preferred_element_type=F32)
        columns = key_positions(s)
        columns = jnp.concatenate([columns] * (2 * rows // 128), axis=1)
        raw = jnp.where(columns <= qpos[0:1], raw, FAR)
        st[s] = raw
        dpt[s] = grad_probs
        before = mx[0:1]
        top = jnp.maximum(before, jnp.max(raw, axis=0, keepdims=True))
        fade = jnp.exp2((before - top) * SCALE2)
        p = jnp.exp2((raw - top) * SCALE2)
        mx[0:1] = top
        tot[0:1] = tot[0:1] * fade + jnp.sum(p, axis=0, keepdims=True)
        dsum[0:1] = dsum[0:1] * fade + jnp.sum(p * grad_probs, axis=0, keepdims=True)

    def side(kind):
        return x + kind - 2 * x * kind

    def at(way, far):
        return lax.rem(z + Z - far, Z) if way == 0 else lax.rem(z + far, Z)

    def sib_number(way, e):
        return 2 + 6 * way + e

    def pass_on(e):
        far, kind = lax.div(e, 2) + 1, lax.rem(e, 2)
        for p in range(PIECES):
            for way in range(2):
                s = dev(side(kind), at(way, far), c)
                arrive(s, p)
                if p // 2 != way:
                    z_copy(way, s, e + 2, p).start()
                else:

                    @pl.when(far <= 2)
                    def _():
                        z_copy(way, s, e + 2, p).start()

                sib_copy(s, sib_number(way, e), p).start()

    def arrive_whole(s):
        for p in range(PIECES):
            arrive(s, p)

    def score_own(e):
        far, kind = lax.div(e, 2) + 1, lax.rem(e, 2)
        for way in range(2):
            scores(dev(side(kind), at(way, far), c))

    def score_sibling(e):
        far, kind = lax.div(e, 2) + 1, lax.rem(e, 2)
        for way in range(2):
            s = dev(side(kind), at(way, far), 1 - c)
            arrive_whole(s)
            scores(s)

    for p in range(PIECES):
        arrive(partner, p)
        z_copy(0, partner, 1, p).start()
        z_copy(1, partner, 1, p).start()
        sib_copy(partner, 1, p).start()
    pass_on(jnp.int32(0))
    for n in range(2):
        loads[7 + n].wait()
        q_copy(n).wait_recv()
    both = jnp.concatenate([key_positions(dev(0, z, c)), key_positions(dev(1, z, c))], axis=0)
    qpos[...] = both.T[0:8]

    def near(kind, carry):
        scores(dev(kind, z, c))
        return carry

    def near_sibling(kind, carry):
        s = dev(side(kind), z, 1 - c)
        arrive_whole(s)
        scores(s)
        return carry

    lax.fori_loop(0, 2, near, 0)
    lax.fori_loop(0, 2, near_sibling, 0)

    def gather_step(e, carry):
        pass_on(e)
        score_own(e - 1)
        score_sibling(e - 1)
        return carry

    lax.fori_loop(1, 6, gather_step, 0)

    def far_pass(kind):
        for p in (2, 0, 3, 1):
            s = dev(side(kind), at(0, 4), c)
            arrive(s, p)
            sib_copy(s, 14 + kind, p).start()

    def far_own(kind, carry):
        scores(dev(side(kind), at(0, 4), c))
        return carry

    def far_sibling(kind, carry):
        s = dev(side(kind), at(0, 4), 1 - c)
        arrive_whole(s)
        scores(s)
        return carry

    far_pass(0)
    score_own(jnp.int32(5))
    score_sibling(jnp.int32(5))
    far_pass(1)
    lax.fori_loop(0, 2, far_own, 0)
    lax.fori_loop(0, 2, far_sibling, 0)

    total = tot[0:1]
    mx[0:1] = mx[0:1] * SCALE2 + jnp.log2(total)
    dsum[0:1] = dsum[0:1] / total

    def grads(s):
        p = jnp.exp2(st[s] * SCALE2 - mx[0:1])
        grad_scores = (p * (dpt[s] - dsum[0:1])).astype(BF16)
        dv = jnp.dot(p.astype(BF16), gf[...], preferred_element_type=F32)
        dk = jnp.dot(grad_scores, qf[...], preferred_element_type=F32) * SCALE
        dqt[...] += lax.dot_general(kvg[s, keys], grad_scores, TN, preferred_element_type=F32)
        return dv, dk

    def g_copy(n):
        return push(sibs.at[n], sibr.at[n], g_send.at[n], g_recv.at[n], sibling)

    def r_copy(way, h, p):
        return push(snd.at[way, h, p], rcv.at[way, h, p], r_send.at[way, h, p], r_recv.at[way, h, p], (up, down)[way])

    def for_sibling(s, n):
        for p, term in enumerate(grads(s)):
            sibs[n, p] = term.astype(BF16)
        g_copy(n).start()

    def for_own(s, h, way):
        for p, term in enumerate(grads(s)):
            part[h, way, p] = term

    def farthest_sibling(h, carry):
        for_sibling(dev(side(1 - h), at(1, 4), 1 - c), h)
        return carry

    def farthest(h, carry):
        for_own(dev(side(1 - h), at(1, 4), c), h, 0)
        g_copy(h).wait_recv()
        for way in range(2):
            p = 1 - way
            snd[way, h, p] = (part[h, 0, p] + sibr[h, p].astype(F32)).astype(BF16)
            r_copy(way, h, p).start()
        return carry

    lax.fori_loop(0, 2, farthest_sibling, 0)
    lax.fori_loop(0, 2, farthest, 0)

    def step_terms(h):
        far = 4 - lax.div(h, 2)
        for way in range(2):
            xx = side(jnp.where(h == 8, 1 - way, 1 - lax.rem(h, 2)))
            for_sibling(dev(xx, at(1 - way, far), 1 - c), 2 * h - 2 + way)
        for way in range(2):
            xx = side(jnp.where(h == 8, 1 - way, 1 - lax.rem(h, 2)))
            for_own(dev(xx, at(1 - way, far), c), h, way)

    def here(h, way, p):
        return part[h, way, p] + sibr[2 * h - 2 + way, p].astype(F32)

    def send_first(h):
        for way in range(2):
            g_copy(2 * h - 2 + way).wait_recv()
            snd[way, h, way] = here(h, way, way).astype(BF16)
            r_copy(way, h, way).start()

    def send_summed(h, turn):
        for way in range(2):
            p = turn if way == 0 else 1 - turn
            r_copy(way, h - 2, p).wait_recv()
            snd[way, h, p] = (here(h, way, p) + rcv[way, h - 2, p].astype(F32)).astype(BF16)
            r_copy(way, h, p).start()

    def send_both(h):
        for way in range(2):
            g_copy(2 * h - 2 + way).wait_recv()
        send_summed(h, 0)
        send_summed(h, 1)

    def first_step(h, carry):
        step_terms(h)
        send_first(h)
        return carry

    lax.fori_loop(2, 4, first_step, 0)

    def reduce_step(h, carry):
        step_terms(h)

        @pl.when(h == 4)
        def _():
            send_summed(jnp.int32(2), 1)
            send_summed(jnp.int32(3), 1)

        @pl.when(jnp.logical_and(h > 4, h < 8))
        def _():
            send_both(h - 1)

        return carry

    lax.fori_loop(4, 9, reduce_step, 0)

    grad_query = dqt[...].T * SCALE
    few = rows // heads
    for n in range(2 * heads):
        dqs[n] = grad_query[n * few : (n + 1) * few].astype(BF16)
    column = hd * 2 + x

    def d_copy(r):
        xx, gg = peer(r)
        n = xx * heads + gg
        return push(dqs.at[n], dqr.at[column], d_send.at[n], d_recv.at[column], dev(xx, z, c), gg)

    def d_wait(r):
        xx, gg = peer(r)
        source = gg * 2 + xx
        return push(dqs.at[0], dqr.at[source], d_send.at[0], d_recv.at[source], dev(xx, z, c), gg)

    @pl.when(c == 0)
    def _():
        pl.semaphore_wait(barrier, 2 * heads - 2)
        signal(far_sem, sibling)

    @pl.when(c == 1)
    def _():
        pl.semaphore_wait(far_sem, 1)

    for r in range(1, 2 * heads):
        d_copy(r).start()
    dqr[column] = dqs[flat]
    send_both(jnp.int32(7))
    for h in range(2):
        g_copy(14 + h).wait_recv()

    def final(h, p):
        for way in range(2):
            r_copy(way, 6 + h, p).wait_recv()
        terms = part[8, h, p] + sibr[14 + h, p].astype(F32)
        return (terms + rcv[0, 6 + h, p].astype(F32) + rcv[1, 6 + h, p].astype(F32)).astype(BF16)

    def xr_copy(p):
        return push(xs.at[p], xr.at[p], xr_send.at[p], xr_recv.at[p], across)

    outs = (dv_ref, dk_ref)
    for p in range(2):
        xs[p] = final(0, p)
        xr_copy(p).start()
    for p in range(2):
        outs[p][:, pl.ds(mine, 128)] = final(1, p)
    for r in range(1, 2 * heads):
        d_wait(r).wait_recv()
    for n in range(2 * heads):
        dq_ref[:, n * 128 : (n + 1) * 128] = dqr[n]

    for way in range(2):
        for p in range(PIECES):
            z_copy(way, me, 0, p).wait_send()
            z_copy(way, partner, 1, p).wait_send()

    def drain_gather(e, carry):
        for way in range(2):
            for p in range(PIECES):
                if p // 2 != way:
                    z_copy(way, me, e + 2, p).wait_send()
                else:

                    @pl.when(e < 4)
                    def _():
                        z_copy(way, me, e + 2, p).wait_send()

            for p in range(2):
                r_copy(way, e + 2, p).wait_send()
        return carry

    lax.fori_loop(0, 6, drain_gather, 0)

    def drain_sibling(n, carry):
        for p in range(PIECES):
            sib_copy(me, n, p).wait_send()
        g_copy(n).wait_send()
        return carry

    lax.fori_loop(0, 16, drain_sibling, 0)
    for h in range(2):
        r_copy(0, h, 1).wait_send()
        r_copy(1, h, 0).wait_send()
        x_copy(h).wait_send()
        x_copy(2 + h).wait_send()
        q_copy(h).wait_send()
    for r in range(1, 2 * heads):
        d_copy(r).wait_send()
    for p in range(2):
        xr_copy(p).wait_recv()
        outs[p][:, pl.ds(other, 128)] = xr[p]
        xr_copy(p).wait_send()


def store(dq_ref, dk_ref, dv_ref, dq_out, dk_out, dv_out, sems):
    pairs = ((dq_ref, dq_out), (dk_ref, dk_out), (dv_ref, dv_out))
    copies = [pltpu.make_async_copy(src, dst, sems.at[n]) for n, (src, dst) in enumerate(pairs)]
    for copy in copies:
        copy.start()
    for copy in copies:
        copy.wait()


def local(query_rows, key_rows, value_rows, grad_output, positions):
    rows, width = query_rows.shape
    heads = lax.axis_size("head")
    members = lax.axis_size("seq")
    vmem = pl.BlockSpec(memory_space=pltpu.VMEM)
    dma, tall = pltpu.SemaphoreType.DMA, 2 * rows + 8
    few = rows // heads
    held = pl.pallas_call(
        kernel,
        out_shape=(
            pltpu.VMEM((few, heads * width), BF16),
            pltpu.VMEM((rows, width), BF16),
            pltpu.VMEM((rows, width), BF16),
        ),
        in_specs=[pl.BlockSpec(memory_space=pl.ANY)] * 5,
        out_specs=(vmem,) * 3,
        scratch_shapes=[
            pltpu.VMEM((members, tall, 128), BF16),
            pltpu.VMEM((tall, 128), BF16),
            pltpu.VMEM((2, rows, 128), BF16),
            pltpu.VMEM((2 * rows, 128), BF16),
            pltpu.VMEM((2 * rows, 128), BF16),
            pltpu.VMEM((1, rows), jnp.int32),
            pltpu.VMEM((8, 128), F32),
            pltpu.VMEM((members, rows, 2 * rows), F32),
            pltpu.VMEM((members, rows, 2 * rows), F32),
            pltpu.VMEM((8, 2 * rows), F32),
            pltpu.VMEM((8, 2 * rows), F32),
            pltpu.VMEM((8, 2 * rows), F32),
            pltpu.VMEM((8, 2 * rows), F32),
            pltpu.VMEM((128, 2 * rows), F32),
            pltpu.VMEM((16, 2, rows, 128), BF16),
            pltpu.VMEM((16, 2, rows, 128), BF16),
            pltpu.VMEM((9, 2, 2, rows, 128), F32),
            pltpu.VMEM((2, 8, 2, rows, 128), BF16),
            pltpu.VMEM((2, 8, 2, rows, 128), BF16),
            pltpu.VMEM((2, rows, 128), BF16),
            pltpu.VMEM((2, rows, 128), BF16),
            pltpu.VMEM((2 * heads, few, 128), BF16),
            pltpu.VMEM((2 * heads, few, 128), BF16),
            dma((9,)),
            dma((members, PIECES)),
            dma((2, 8, PIECES)),
            dma((16, PIECES)),
            dma((PIECES + 2,)),
            dma((2,)),
            dma((16,)),
            dma((16,)),
            dma((2, 8, 2)),
            dma((2, 8, 2)),
            dma((2,)),
            dma((2,)),
            dma((2 * heads,)),
            dma((2 * heads,)),
            pltpu.SemaphoreType.REGULAR,
            pltpu.SemaphoreType.REGULAR,
            pltpu.SemaphoreType.REGULAR,
        ],
        compiler_params=pltpu.CompilerParams(
            collective_id=0, has_side_effects=True, vmem_limit_bytes=60 * 1024 * 1024
        ),
    )(query_rows, key_rows, value_rows, grad_output, positions.reshape(1, rows))
    held = [pltpu.with_memory_space_constraint(h, pltpu.VMEM) for h in held]
    return pl.pallas_call(
        store,
        out_shape=tuple(jax.ShapeDtypeStruct(h.shape, h.dtype) for h in held),
        in_specs=[vmem] * 3,
        out_specs=(pl.BlockSpec(memory_space=pl.ANY),) * 3,
        scratch_shapes=[dma((3,))],
    )(*held)


def solution(mesh):
    placed = (P("seq", "head"), P("seq", "head"), P("seq", "head"), P("seq", "head"), P("seq"))
    return jax.shard_map(
        local,
        mesh=mesh,
        in_specs=placed,
        out_specs=(P(("seq", "head"), None), P("seq", "head"), P("seq", "head")),
        check_vma=False,
    )
```

```python
import math

import jax
import jax.numpy as jnp
from jax import lax
from jax.experimental import pallas as pl
from jax.experimental.pallas import tpu as pltpu
from jax.sharding import PartitionSpec as P

MESH = pl.DeviceIdType.MESH
HEAD_DIM = 128
SCALE = HEAD_DIM**-0.5
SCALE2 = SCALE * math.log2(math.e)
FAR = -1e30
Z = 8
PIECES = 4
F32, BF16 = jnp.float32, jnp.bfloat16
NT = (((1,), (1,)), ((), ()))
TN = (((0,), (0,)), ((), ()))


def kernel(
    q_ref, k_ref, v_ref, g_ref, pos_ref, dq_ref, dk_ref, dv_ref,
    kvg, xkv, xq, qf, gf, posr, posb, st, dpt, qpos, mx, tot, dsum, dqt,
    sibs, sibr, part, snd, rcv, xs, xr, dqs, dqr,
    l_sem, in_recv, z_send, sib_send, x_send, q_recv, g_send, g_recv,
    r_send, r_recv, xr_send, xr_recv, d_send, d_recv, go_sem, far_sem,
):
    rows = q_ref.shape[0]
    me, hd = lax.axis_index("seq"), lax.axis_index("head")
    heads = lax.axis_size("head")
    x, z, c = lax.div(me, 16), lax.div(lax.rem(me, 16), 2), lax.rem(me, 2)

    def dev(xx, zz, cc):
        return xx * 16 + zz * 2 + cc

    up, down = dev(x, lax.rem(z + 1, Z), c), dev(x, lax.rem(z + Z - 1, Z), c)
    sibling, across = dev(x, z, 1 - c), dev(1 - x, z, c)
    partner = across

    def push(src, dst, send, recv, seq, head=hd):
        return pltpu.make_async_remote_copy(
            src_ref=src, dst_ref=dst, send_sem=send, recv_sem=recv,
            device_id={"seq": seq, "head": head}, device_id_type=MESH,
        )

    vals, keys, tail = pl.ds(0, rows), pl.ds(rows, rows), pl.ds(2 * rows, 8)
    some = rows // 2
    cut = (pl.ds(0, some), pl.ds(some, some), pl.ds(rows, some), pl.ds(rows + some, some + 8))

    mine, other = pl.multiple_of(x * 128, 128), pl.multiple_of((1 - x) * 128, 128)
    held = pl.ds(pl.multiple_of(x * rows, rows), rows)
    loads = [
        pltpu.make_async_copy(src, dst, l_sem.at[n])
        for n, (src, dst) in enumerate((
            (pos_ref, posr),
            (v_ref.at[:, pl.ds(mine, 128)], kvg.at[me, vals]),
            (v_ref.at[:, pl.ds(other, 128)], xkv.at[vals]),
            (k_ref.at[:, pl.ds(mine, 128)], kvg.at[me, keys]),
            (k_ref.at[:, pl.ds(other, 128)], xkv.at[keys]),
            (q_ref.at[:, pl.ds(other, 128)], xq.at[0]),
            (g_ref.at[:, pl.ds(other, 128)], xq.at[1]),
            (q_ref.at[:, pl.ds(mine, 128)], qf.at[held]),
            (g_ref.at[:, pl.ds(mine, 128)], gf.at[held]),
        ))
    ]
    for load in loads:
        load.start()

    flat = x * heads + hd

    def peer(r):
        there = lax.rem(flat + r, 2 * heads)
        return lax.div(there, heads), lax.rem(there, heads)

    barrier = pltpu.get_barrier_semaphore()

    def signal(sem, seq, head=hd):
        pl.semaphore_signal(sem, inc=1, device_id={"seq": seq, "head": head}, device_id_type=MESH)

    near_by = (up, down, across, sibling)
    for seq in near_by:

        @pl.when(seq != 0)
        def _():
            signal(barrier, seq)

    mx[...] = jnp.full(mx.shape, FAR, F32)
    tot[...] = jnp.zeros(tot.shape, F32)
    dsum[...] = jnp.zeros(dsum.shape, F32)
    dqt[...] = jnp.zeros(dqt.shape, F32)

    loads[0].wait()
    place = posr[...].astype(F32)
    high = jnp.floor(place * (1.0 / 64.0))
    low = place - 64.0 * high
    posb[...] = jnp.zeros(posb.shape, F32)
    for n, digit in enumerate((high, low)):
        posb[2 * n : 2 * n + 1, :] = digit[:, 0:128]
        posb[2 * n + 1 : 2 * n + 2, 0 : rows - 128] = digit[:, 128:rows]
    kvg[me, tail] = posb[...].astype(BF16)
    xkv[tail] = posb[...].astype(BF16)

    @pl.when(me != 0)
    def _():
        pl.semaphore_wait(barrier, 4)
        for seq in near_by:

            @pl.when(seq == 0)
            def _():
                signal(go_sem, seq)

    @pl.when(me == 0)
    def _():
        pl.semaphore_wait(go_sem, 4)

    def z_copy(way, s, n, p):
        return push(kvg.at[s, cut[p]], kvg.at[s, cut[p]], z_send.at[way, n, p], in_recv.at[s, p], (up, down)[way])

    def sib_copy(s, n, p):
        return push(kvg.at[s, cut[p]], kvg.at[s, cut[p]], sib_send.at[n, p], in_recv.at[s, p], sibling)

    def x_copy(p):
        return push(xkv.at[cut[p]], kvg.at[me, cut[p]], x_send.at[p], in_recv.at[me, p], across)

    def q_copy(n):
        return push(xq.at[n], (qf, gf)[n].at[held], x_send.at[4 + n], q_recv.at[n], across)

    for half in range(2):
        loads[1 + 2 * half].wait()
        loads[2 + 2 * half].wait()
        for p in (2 * half, 2 * half + 1):
            z_copy(0, me, 0, p).start()
            z_copy(1, me, 0, p).start()
            x_copy(p).start()
        for p in (2 * half, 2 * half + 1):
            sib_copy(me, 0, p).start()
    for n in range(2):
        loads[5 + n].wait()
        q_copy(n).start()

    def arrive(s, p):
        sib_copy(s, 0, p).wait_recv()

    def key_positions(s):
        block = kvg[s, 2 * rows : 2 * rows + 8].astype(F32)
        first = block[0:1] * 64.0 + block[2:3]
        rest = block[1:2] * 64.0 + block[3:4]
        return jnp.concatenate(
            [jnp.broadcast_to(first, (128, 128)).T, jnp.broadcast_to(rest, (128, 128)).T[0 : rows - 128]], axis=0
        )

    def scores(s):
        raw = lax.dot_general(kvg[s, keys], qf[...], NT, preferred_element_type=F32)
        grad_probs = lax.dot_general(kvg[s, vals], gf[...], NT, preferred_element_type=F32)
        columns = key_positions(s)
        columns = jnp.concatenate([columns] * (2 * rows // 128), axis=1)
        raw = jnp.where(columns <= qpos[0:1], raw, FAR)
        st[s] = raw
        dpt[s] = grad_probs
        before = mx[0:1]
        top = jnp.maximum(before, jnp.max(raw, axis=0, keepdims=True))
        fade = jnp.exp2((before - top) * SCALE2)
        p = jnp.exp2((raw - top) * SCALE2)
        mx[0:1] = top
        tot[0:1] = tot[0:1] * fade + jnp.sum(p, axis=0, keepdims=True)
        dsum[0:1] = dsum[0:1] * fade + jnp.sum(p * grad_probs, axis=0, keepdims=True)

    def side(kind):
        return x + kind - 2 * x * kind

    def at(way, far):
        return lax.rem(z + Z - far, Z) if way == 0 else lax.rem(z + far, Z)

    def sib_number(way, e):
        return 2 + 6 * way + e

    def pass_on(e):
        far, kind = lax.div(e, 2) + 1, lax.rem(e, 2)
        for p in range(PIECES):
            for way in range(2):
                s = dev(side(kind), at(way, far), c)
                arrive(s, p)
                if p // 2 != way:
                    z_copy(way, s, e + 2, p).start()
                else:

                    @pl.when(far <= 2)
                    def _():
                        z_copy(way, s, e + 2, p).start()

                sib_copy(s, sib_number(way, e), p).start()

    def arrive_whole(s):
        for p in range(PIECES):
            arrive(s, p)

    def score_own(e):
        far, kind = lax.div(e, 2) + 1, lax.rem(e, 2)
        for way in range(2):
            scores(dev(side(kind), at(way, far), c))

    def score_sibling(e):
        far, kind = lax.div(e, 2) + 1, lax.rem(e, 2)
        for way in range(2):
            s = dev(side(kind), at(way, far), 1 - c)
            arrive_whole(s)
            scores(s)

    for p in range(PIECES):
        arrive(partner, p)
        z_copy(0, partner, 1, p).start()
        z_copy(1, partner, 1, p).start()
        sib_copy(partner, 1, p).start()
    pass_on(jnp.int32(0))
    for n in range(2):
        loads[7 + n].wait()
        q_copy(n).wait_recv()
    both = jnp.concatenate([key_positions(dev(0, z, c)), key_positions(dev(1, z, c))], axis=0)
    qpos[...] = both.T[0:8]

    def near(kind, carry):
        scores(dev(kind, z, c))
        return carry

    def near_sibling(kind, carry):
        s = dev(side(kind), z, 1 - c)
        arrive_whole(s)
        scores(s)
        return carry

    lax.fori_loop(0, 2, near, 0)
    lax.fori_loop(0, 2, near_sibling, 0)

    def gather_step(e, carry):
        pass_on(e)
        score_own(e - 1)
        score_sibling(e - 1)
        return carry

    lax.fori_loop(1, 6, gather_step, 0)

    def far_pass(kind):
        for p in (2, 0, 3, 1):
            s = dev(side(kind), at(0, 4), c)
            arrive(s, p)
            sib_copy(s, 14 + kind, p).start()

    def far_own(kind, carry):
        scores(dev(side(kind), at(0, 4), c))
        return carry

    def far_sibling(kind, carry):
        s = dev(side(kind), at(0, 4), 1 - c)
        arrive_whole(s)
        scores(s)
        return carry

    far_pass(0)
    score_own(jnp.int32(5))
    score_sibling(jnp.int32(5))
    far_pass(1)
    lax.fori_loop(0, 2, far_own, 0)
    lax.fori_loop(0, 2, far_sibling, 0)

    @pl.when(me == 0)
    def _():
        for r in range(1, heads):
            signal(barrier, me, lax.rem(hd + r, heads))

    total = tot[0:1]
    mx[0:1] = mx[0:1] * SCALE2 + jnp.log2(total)
    dsum[0:1] = dsum[0:1] / total

    def grads(s):
        p = jnp.exp2(st[s] * SCALE2 - mx[0:1])
        grad_scores = (p * (dpt[s] - dsum[0:1])).astype(BF16)
        dv = jnp.dot(p.astype(BF16), gf[...], preferred_element_type=F32)
        dk = jnp.dot(grad_scores, qf[...], preferred_element_type=F32) * SCALE
        dqt[...] += lax.dot_general(kvg[s, keys], grad_scores, TN, preferred_element_type=F32)
        return dv, dk

    def g_copy(n):
        return push(sibs.at[n], sibr.at[n], g_send.at[n], g_recv.at[n], sibling)

    def r_copy(way, h, p):
        return push(snd.at[way, h, p], rcv.at[way, h, p], r_send.at[way, h, p], r_recv.at[way, h, p], (up, down)[way])

    def for_sibling(s, n):
        for p, term in enumerate(grads(s)):
            sibs[n, p] = term.astype(BF16)
        g_copy(n).start()

    def for_own(s, h, way):
        for p, term in enumerate(grads(s)):
            part[h, way, p] = term

    def farthest_sibling(h, carry):
        for_sibling(dev(side(1 - h), at(1, 4), 1 - c), h)
        return carry

    def farthest(h, carry):
        for_own(dev(side(1 - h), at(1, 4), c), h, 0)
        g_copy(h).wait_recv()
        for way in range(2):
            p = 1 - way
            snd[way, h, p] = (part[h, 0, p] + sibr[h, p].astype(F32)).astype(BF16)
            r_copy(way, h, p).start()
        return carry

    lax.fori_loop(0, 2, farthest_sibling, 0)
    lax.fori_loop(0, 2, farthest, 0)

    def step_terms(h):
        far = 4 - lax.div(h, 2)
        for way in range(2):
            xx = side(jnp.where(h == 8, 1 - way, 1 - lax.rem(h, 2)))
            for_sibling(dev(xx, at(1 - way, far), 1 - c), 2 * h - 2 + way)
        for way in range(2):
            xx = side(jnp.where(h == 8, 1 - way, 1 - lax.rem(h, 2)))
            for_own(dev(xx, at(1 - way, far), c), h, way)

    def here(h, way, p):
        return part[h, way, p] + sibr[2 * h - 2 + way, p].astype(F32)

    def send_first(h):
        for way in range(2):
            g_copy(2 * h - 2 + way).wait_recv()
            snd[way, h, way] = here(h, way, way).astype(BF16)
            r_copy(way, h, way).start()

    def send_summed(h, turn):
        for way in range(2):
            p = turn if way == 0 else 1 - turn
            r_copy(way, h - 2, p).wait_recv()
            snd[way, h, p] = (here(h, way, p) + rcv[way, h - 2, p].astype(F32)).astype(BF16)
            r_copy(way, h, p).start()

    def send_both(h):
        for way in range(2):
            g_copy(2 * h - 2 + way).wait_recv()
        send_summed(h, 0)
        send_summed(h, 1)

    def first_step(h, carry):
        step_terms(h)
        send_first(h)
        return carry

    lax.fori_loop(2, 4, first_step, 0)

    def reduce_step(h, carry):
        @pl.when(jnp.logical_and(h == 6, me == 0))
        def _():
            pl.semaphore_wait(barrier, heads - 1)

            def tell(n, carry):
                signal(far_sem, n)
                return carry

            lax.fori_loop(1, lax.axis_size("seq"), tell, 0)

        step_terms(h)

        @pl.when(h == 4)
        def _():
            send_summed(jnp.int32(2), 1)
            send_summed(jnp.int32(3), 1)

        @pl.when(jnp.logical_and(h > 4, h < 8))
        def _():
            send_both(h - 1)

        return carry

    lax.fori_loop(4, 9, reduce_step, 0)

    grad_query = dqt[...].T * SCALE
    few = rows // heads
    for n in range(2 * heads):
        dqs[n] = grad_query[n * few : (n + 1) * few].astype(BF16)
    column = hd * 2 + x

    def d_copy(r):
        xx, gg = peer(r)
        n = xx * heads + gg
        return push(dqs.at[n], dqr.at[column], d_send.at[n], d_recv.at[column], dev(xx, z, c), gg)

    def d_wait(r):
        xx, gg = peer(r)
        source = gg * 2 + xx
        return push(dqs.at[0], dqr.at[source], d_send.at[0], d_recv.at[source], dev(xx, z, c), gg)

    @pl.when(me != 0)
    def _():
        pl.semaphore_wait(far_sem, 1)

    for r in range(1, 2 * heads):
        d_copy(r).start()
    dqr[column] = dqs[flat]
    send_both(jnp.int32(7))
    for h in range(2):
        g_copy(14 + h).wait_recv()

    def final(h, p):
        for way in range(2):
            r_copy(way, 6 + h, p).wait_recv()
        terms = part[8, h, p] + sibr[14 + h, p].astype(F32)
        return (terms + rcv[0, 6 + h, p].astype(F32) + rcv[1, 6 + h, p].astype(F32)).astype(BF16)

    def xr_copy(p):
        return push(xs.at[p], xr.at[p], xr_send.at[p], xr_recv.at[p], across)

    outs = (dv_ref, dk_ref)
    for p in range(2):
        xs[p] = final(0, p)
        xr_copy(p).start()
    for p in range(2):
        outs[p][:, pl.ds(mine, 128)] = final(1, p)
    for r in range(1, 2 * heads):
        d_wait(r).wait_recv()
    for n in range(2 * heads):
        dq_ref[:, n * 128 : (n + 1) * 128] = dqr[n]

    for way in range(2):
        for p in range(PIECES):
            z_copy(way, me, 0, p).wait_send()
            z_copy(way, partner, 1, p).wait_send()

    def drain_gather(e, carry):
        for way in range(2):
            for p in range(PIECES):
                if p // 2 != way:
                    z_copy(way, me, e + 2, p).wait_send()
                else:

                    @pl.when(e < 4)
                    def _():
                        z_copy(way, me, e + 2, p).wait_send()

            for p in range(2):
                r_copy(way, e + 2, p).wait_send()
        return carry

    lax.fori_loop(0, 6, drain_gather, 0)

    def drain_sibling(n, carry):
        for p in range(PIECES):
            sib_copy(me, n, p).wait_send()
        g_copy(n).wait_send()
        return carry

    lax.fori_loop(0, 16, drain_sibling, 0)
    for h in range(2):
        r_copy(0, h, 1).wait_send()
        r_copy(1, h, 0).wait_send()
        x_copy(h).wait_send()
        x_copy(2 + h).wait_send()
        q_copy(h).wait_send()
    for r in range(1, 2 * heads):
        d_copy(r).wait_send()
    for p in range(2):
        xr_copy(p).wait_recv()
        outs[p][:, pl.ds(other, 128)] = xr[p]
        xr_copy(p).wait_send()


def store(dq_ref, dk_ref, dv_ref, dq_out, dk_out, dv_out, sems):
    pairs = ((dq_ref, dq_out), (dk_ref, dk_out), (dv_ref, dv_out))
    copies = [pltpu.make_async_copy(src, dst, sems.at[n]) for n, (src, dst) in enumerate(pairs)]
    for copy in copies:
        copy.start()
    for copy in copies:
        copy.wait()


def local(query_rows, key_rows, value_rows, grad_output, positions):
    rows, width = query_rows.shape
    heads = lax.axis_size("head")
    members = lax.axis_size("seq")
    vmem = pl.BlockSpec(memory_space=pltpu.VMEM)
    dma, tall = pltpu.SemaphoreType.DMA, 2 * rows + 8
    few = rows // heads
    held = pl.pallas_call(
        kernel,
        out_shape=(
            pltpu.VMEM((few, heads * width), BF16),
            pltpu.VMEM((rows, width), BF16),
            pltpu.VMEM((rows, width), BF16),
        ),
        in_specs=[pl.BlockSpec(memory_space=pl.ANY)] * 5,
        out_specs=(vmem,) * 3,
        scratch_shapes=[
            pltpu.VMEM((members, tall, 128), BF16),
            pltpu.VMEM((tall, 128), BF16),
            pltpu.VMEM((2, rows, 128), BF16),
            pltpu.VMEM((2 * rows, 128), BF16),
            pltpu.VMEM((2 * rows, 128), BF16),
            pltpu.VMEM((1, rows), jnp.int32),
            pltpu.VMEM((8, 128), F32),
            pltpu.VMEM((members, rows, 2 * rows), F32),
            pltpu.VMEM((members, rows, 2 * rows), F32),
            pltpu.VMEM((8, 2 * rows), F32),
            pltpu.VMEM((8, 2 * rows), F32),
            pltpu.VMEM((8, 2 * rows), F32),
            pltpu.VMEM((8, 2 * rows), F32),
            pltpu.VMEM((128, 2 * rows), F32),
            pltpu.VMEM((16, 2, rows, 128), BF16),
            pltpu.VMEM((16, 2, rows, 128), BF16),
            pltpu.VMEM((9, 2, 2, rows, 128), F32),
            pltpu.VMEM((2, 8, 2, rows, 128), BF16),
            pltpu.VMEM((2, 8, 2, rows, 128), BF16),
            pltpu.VMEM((2, rows, 128), BF16),
            pltpu.VMEM((2, rows, 128), BF16),
            pltpu.VMEM((2 * heads, few, 128), BF16),
            pltpu.VMEM((2 * heads, few, 128), BF16),
            dma((9,)),
            dma((members, PIECES)),
            dma((2, 8, PIECES)),
            dma((16, PIECES)),
            dma((PIECES + 2,)),
            dma((2,)),
            dma((16,)),
            dma((16,)),
            dma((2, 8, 2)),
            dma((2, 8, 2)),
            dma((2,)),
            dma((2,)),
            dma((2 * heads,)),
            dma((2 * heads,)),
            pltpu.SemaphoreType.REGULAR,
            pltpu.SemaphoreType.REGULAR,
        ],
        compiler_params=pltpu.CompilerParams(
            collective_id=0, has_side_effects=True, vmem_limit_bytes=60 * 1024 * 1024
        ),
    )(query_rows, key_rows, value_rows, grad_output, positions.reshape(1, rows))
    held = [pltpu.with_memory_space_constraint(h, pltpu.VMEM) for h in held]
    return pl.pallas_call(
        store,
        out_shape=tuple(jax.ShapeDtypeStruct(h.shape, h.dtype) for h in held),
        in_specs=[vmem] * 3,
        out_specs=(pl.BlockSpec(memory_space=pl.ANY),) * 3,
        scratch_shapes=[dma((3,))],
    )(*held)


def solution(mesh):
    placed = (P("seq", "head"), P("seq", "head"), P("seq", "head"), P("seq", "head"), P("seq"))
    return jax.shard_map(
        local,
        mesh=mesh,
        in_specs=placed,
        out_specs=(P(("seq", "head"), None), P("seq", "head"), P("seq", "head")),
        check_vma=False,
    )
```

```python
import math

import jax
import jax.numpy as jnp
from jax import lax
from jax.experimental import pallas as pl
from jax.experimental.pallas import tpu as pltpu
from jax.sharding import PartitionSpec as P

MESH = pl.DeviceIdType.MESH
HEAD_DIM = 128
SCALE = HEAD_DIM**-0.5
SCALE2 = SCALE * math.log2(math.e)
FAR = -1e30
Z = 8
PIECES = 4
F32, BF16 = jnp.float32, jnp.bfloat16
NT = (((1,), (1,)), ((), ()))
TN = (((0,), (0,)), ((), ()))


def kernel(
    q_ref, k_ref, v_ref, g_ref, pos_ref, dq_ref, dk_ref, dv_ref,
    kvg, xkv, xq, qf, gf, posr, posb, st, dpt, qpos, mx, tot, dsum, dqt,
    sibs, sibr, part, snd, rcv, xs, xr, dqs, dqr,
    l_sem, in_recv, z_send, sib_send, x_send, q_recv, g_send, g_recv,
    r_send, r_recv, xr_send, xr_recv, d_send, d_recv, go_sem, far_sem,
):
    rows = q_ref.shape[0]
    me, hd = lax.axis_index("seq"), lax.axis_index("head")
    heads = lax.axis_size("head")
    x, z, c = lax.div(me, 16), lax.div(lax.rem(me, 16), 2), lax.rem(me, 2)

    def dev(xx, zz, cc):
        return xx * 16 + zz * 2 + cc

    up, down = dev(x, lax.rem(z + 1, Z), c), dev(x, lax.rem(z + Z - 1, Z), c)
    sibling, across = dev(x, z, 1 - c), dev(1 - x, z, c)
    partner = across

    def push(src, dst, send, recv, seq, head=hd):
        return pltpu.make_async_remote_copy(
            src_ref=src, dst_ref=dst, send_sem=send, recv_sem=recv,
            device_id={"seq": seq, "head": head}, device_id_type=MESH,
        )

    vals, keys, tail = pl.ds(0, rows), pl.ds(rows, rows), pl.ds(2 * rows, 8)
    some = rows // 2
    cut = (pl.ds(0, some), pl.ds(some, some), pl.ds(rows, some), pl.ds(rows + some, some + 8))

    mine, other = pl.multiple_of(x * 128, 128), pl.multiple_of((1 - x) * 128, 128)
    held = pl.ds(pl.multiple_of(x * rows, rows), rows)
    loads = [
        pltpu.make_async_copy(src, dst, l_sem.at[n])
        for n, (src, dst) in enumerate((
            (pos_ref, posr),
            (v_ref.at[:, pl.ds(mine, 128)], kvg.at[me, vals]),
            (v_ref.at[:, pl.ds(other, 128)], xkv.at[vals]),
            (k_ref.at[:, pl.ds(mine, 128)], kvg.at[me, keys]),
            (k_ref.at[:, pl.ds(other, 128)], xkv.at[keys]),
            (q_ref.at[:, pl.ds(other, 128)], xq.at[0]),
            (g_ref.at[:, pl.ds(other, 128)], xq.at[1]),
            (q_ref.at[:, pl.ds(mine, 128)], qf.at[held]),
            (g_ref.at[:, pl.ds(mine, 128)], gf.at[held]),
        ))
    ]
    for load in loads:
        load.start()

    flat = x * heads + hd

    def peer(r):
        there = lax.rem(flat + r, 2 * heads)
        return lax.div(there, heads), lax.rem(there, heads)

    barrier = pltpu.get_barrier_semaphore()

    def signal(sem, seq, head=hd):
        pl.semaphore_signal(sem, inc=1, device_id={"seq": seq, "head": head}, device_id_type=MESH)

    near_by = (up, down, across, sibling)
    for seq in near_by:

        @pl.when(seq != 0)
        def _():
            signal(barrier, seq)

    mx[...] = jnp.full(mx.shape, FAR, F32)
    tot[...] = jnp.zeros(tot.shape, F32)
    dsum[...] = jnp.zeros(dsum.shape, F32)
    dqt[...] = jnp.zeros(dqt.shape, F32)

    loads[0].wait()
    place = posr[...].astype(F32)
    high = jnp.floor(place * (1.0 / 64.0))
    low = place - 64.0 * high
    posb[...] = jnp.zeros(posb.shape, F32)
    for n, digit in enumerate((high, low)):
        posb[2 * n : 2 * n + 1, :] = digit[:, 0:128]
        posb[2 * n + 1 : 2 * n + 2, 0 : rows - 128] = digit[:, 128:rows]
    kvg[me, tail] = posb[...].astype(BF16)
    xkv[tail] = posb[...].astype(BF16)

    @pl.when(me != 0)
    def _():
        pl.semaphore_wait(barrier, 4)
        for seq in near_by:

            @pl.when(seq == 0)
            def _():
                signal(go_sem, seq)

    @pl.when(me == 0)
    def _():
        pl.semaphore_wait(go_sem, 4)

    def z_copy(way, s, n, p):
        return push(kvg.at[s, cut[p]], kvg.at[s, cut[p]], z_send.at[way, n, p], in_recv.at[s, p], (up, down)[way])

    def sib_copy(s, n, p):
        return push(kvg.at[s, cut[p]], kvg.at[s, cut[p]], sib_send.at[n, p], in_recv.at[s, p], sibling)

    def x_copy(p):
        return push(xkv.at[cut[p]], kvg.at[me, cut[p]], x_send.at[p], in_recv.at[me, p], across)

    def q_copy(n):
        return push(xq.at[n], (qf, gf)[n].at[held], x_send.at[4 + n], q_recv.at[n], across)

    for half in range(2):
        loads[1 + 2 * half].wait()
        loads[2 + 2 * half].wait()
        for p in (2 * half, 2 * half + 1):
            z_copy(0, me, 0, p).start()
            z_copy(1, me, 0, p).start()
            x_copy(p).start()
        for p in (2 * half, 2 * half + 1):
            sib_copy(me, 0, p).start()
    for n in range(2):
        loads[5 + n].wait()
        q_copy(n).start()

    def arrive(s, p):
        sib_copy(s, 0, p).wait_recv()

    def key_positions(s):
        block = kvg[s, 2 * rows : 2 * rows + 8].astype(F32)
        first = block[0:1] * 64.0 + block[2:3]
        rest = block[1:2] * 64.0 + block[3:4]
        return jnp.concatenate(
            [jnp.broadcast_to(first, (128, 128)).T, jnp.broadcast_to(rest, (128, 128)).T[0 : rows - 128]], axis=0
        )

    def scores(s):
        raw = lax.dot_general(kvg[s, keys], qf[...], NT, preferred_element_type=F32)
        grad_probs = lax.dot_general(kvg[s, vals], gf[...], NT, preferred_element_type=F32)
        columns = key_positions(s)
        columns = jnp.concatenate([columns] * (2 * rows // 128), axis=1)
        raw = jnp.where(columns <= qpos[0:1], raw, FAR)
        st[s] = raw
        dpt[s] = grad_probs
        before = mx[0:1]
        top = jnp.maximum(before, jnp.max(raw, axis=0, keepdims=True))
        fade = jnp.exp2((before - top) * SCALE2)
        p = jnp.exp2((raw - top) * SCALE2)
        mx[0:1] = top
        tot[0:1] = tot[0:1] * fade + jnp.sum(p, axis=0, keepdims=True)
        dsum[0:1] = dsum[0:1] * fade + jnp.sum(p * grad_probs, axis=0, keepdims=True)

    def side(kind):
        return x + kind - 2 * x * kind

    def at(way, far):
        return lax.rem(z + Z - far, Z) if way == 0 else lax.rem(z + far, Z)

    def sib_number(way, e):
        return 2 + 6 * way + e

    def pass_on(e):
        far, kind = lax.div(e, 2) + 1, lax.rem(e, 2)
        for p in range(PIECES):
            for way in range(2):
                s = dev(side(kind), at(way, far), c)
                arrive(s, p)
                if p // 2 != way:
                    z_copy(way, s, e + 2, p).start()
                else:

                    @pl.when(far <= 2)
                    def _():
                        z_copy(way, s, e + 2, p).start()

                sib_copy(s, sib_number(way, e), p).start()

    def arrive_whole(s):
        for p in range(PIECES):
            arrive(s, p)

    def score_own(e):
        far, kind = lax.div(e, 2) + 1, lax.rem(e, 2)
        for way in range(2):
            scores(dev(side(kind), at(way, far), c))

    def score_sibling(e):
        far, kind = lax.div(e, 2) + 1, lax.rem(e, 2)
        for way in range(2):
            s = dev(side(kind), at(way, far), 1 - c)
            arrive_whole(s)
            scores(s)

    for p in range(PIECES):
        arrive(partner, p)
        z_copy(0, partner, 1, p).start()
        z_copy(1, partner, 1, p).start()
        sib_copy(partner, 1, p).start()
    pass_on(jnp.int32(0))
    for n in range(2):
        loads[7 + n].wait()
        q_copy(n).wait_recv()
    both = jnp.concatenate([key_positions(dev(0, z, c)), key_positions(dev(1, z, c))], axis=0)
    qpos[...] = both.T[0:8]

    def near(kind, carry):
        scores(dev(kind, z, c))
        return carry

    def near_sibling(kind, carry):
        s = dev(side(kind), z, 1 - c)
        arrive_whole(s)
        scores(s)
        return carry

    lax.fori_loop(0, 2, near, 0)
    lax.fori_loop(0, 2, near_sibling, 0)

    def gather_step(e, carry):
        pass_on(e)
        score_own(e - 1)
        score_sibling(e - 1)
        return carry

    lax.fori_loop(1, 6, gather_step, 0)

    def far_pass(kind):
        for p in (2, 0, 3, 1):
            s = dev(side(kind), at(0, 4), c)
            arrive(s, p)
            sib_copy(s, 14 + kind, p).start()

    def far_own(kind, carry):
        scores(dev(side(kind), at(0, 4), c))
        return carry

    def far_sibling(kind, carry):
        s = dev(side(kind), at(0, 4), 1 - c)
        arrive_whole(s)
        scores(s)
        return carry

    far_pass(0)
    score_own(jnp.int32(5))
    score_sibling(jnp.int32(5))
    far_pass(1)
    lax.fori_loop(0, 2, far_own, 0)
    lax.fori_loop(0, 2, far_sibling, 0)

    @pl.when(me == 0)
    def _():
        for r in range(1, heads):
            signal(barrier, me, lax.rem(hd + r, heads))

    total = tot[0:1]
    mx[0:1] = mx[0:1] * SCALE2 + jnp.log2(total)
    dsum[0:1] = dsum[0:1] / total

    def grads(s):
        p = jnp.exp2(st[s] * SCALE2 - mx[0:1])
        grad_scores = (p * (dpt[s] - dsum[0:1])).astype(BF16)
        dv = jnp.dot(p.astype(BF16), gf[...], preferred_element_type=F32)
        dk = jnp.dot(grad_scores, qf[...], preferred_element_type=F32) * SCALE
        dqt[...] += lax.dot_general(kvg[s, keys], grad_scores, TN, preferred_element_type=F32)
        return dv, dk

    def g_copy(n):
        return push(sibs.at[n], sibr.at[n], g_send.at[n], g_recv.at[n], sibling)

    def r_copy(way, h, p):
        return push(snd.at[way, h, p], rcv.at[way, h, p], r_send.at[way, h, p], r_recv.at[way, h, p], (up, down)[way])

    def for_sibling(s, n):
        for p, term in enumerate(grads(s)):
            sibs[n, p] = term.astype(BF16)
        g_copy(n).start()

    def for_own(s, h, way):
        for p, term in enumerate(grads(s)):
            part[h, way, p] = term

    def farthest_sibling(h, carry):
        for_sibling(dev(side(1 - h), at(1, 4), 1 - c), h)
        return carry

    def farthest(h, carry):
        for_own(dev(side(1 - h), at(1, 4), c), h, 0)
        g_copy(h).wait_recv()
        for way in range(2):
            p = 1 - way
            snd[way, h, p] = (part[h, 0, p] + sibr[h, p].astype(F32)).astype(BF16)
            r_copy(way, h, p).start()
        return carry

    lax.fori_loop(0, 2, farthest_sibling, 0)
    lax.fori_loop(0, 2, farthest, 0)

    def step_terms(h):
        far = 4 - lax.div(h, 2)
        for way in range(2):
            xx = side(jnp.where(h == 8, 1 - way, 1 - lax.rem(h, 2)))
            for_sibling(dev(xx, at(1 - way, far), 1 - c), 2 * h - 2 + way)
        for way in range(2):
            xx = side(jnp.where(h == 8, 1 - way, 1 - lax.rem(h, 2)))
            for_own(dev(xx, at(1 - way, far), c), h, way)

    def here(h, way, p):
        return part[h, way, p] + sibr[2 * h - 2 + way, p].astype(F32)

    def send_first(h):
        for way in range(2):
            g_copy(2 * h - 2 + way).wait_recv()
            snd[way, h, way] = here(h, way, way).astype(BF16)
            r_copy(way, h, way).start()

    def send_summed(h, turn):
        for way in range(2):
            p = turn if way == 0 else 1 - turn
            r_copy(way, h - 2, p).wait_recv()
            snd[way, h, p] = (here(h, way, p) + rcv[way, h - 2, p].astype(F32)).astype(BF16)
            r_copy(way, h, p).start()

    def send_both(h):
        for way in range(2):
            g_copy(2 * h - 2 + way).wait_recv()
        send_summed(h, 0)
        send_summed(h, 1)

    def first_step(h, carry):
        step_terms(h)
        send_first(h)
        return carry

    lax.fori_loop(2, 4, first_step, 0)

    def reduce_step(h, carry):
        @pl.when(jnp.logical_and(h == 5, me == 0))
        def _():
            pl.semaphore_wait(barrier, heads - 1)

            def tell(n, carry):
                signal(far_sem, n)
                return carry

            lax.fori_loop(1, lax.axis_size("seq"), tell, 0)

        step_terms(h)

        @pl.when(h == 4)
        def _():
            send_summed(jnp.int32(2), 1)
            send_summed(jnp.int32(3), 1)

        @pl.when(jnp.logical_and(h > 4, h < 8))
        def _():
            send_both(h - 1)

        return carry

    lax.fori_loop(4, 9, reduce_step, 0)

    grad_query = dqt[...].T * SCALE
    few = rows // heads
    for n in range(2 * heads):
        dqs[n] = grad_query[n * few : (n + 1) * few].astype(BF16)
    column = hd * 2 + x

    def d_copy(r):
        xx, gg = peer(r)
        n = xx * heads + gg
        return push(dqs.at[n], dqr.at[column], d_send.at[n], d_recv.at[column], dev(xx, z, c), gg)

    def d_wait(r):
        xx, gg = peer(r)
        source = gg * 2 + xx
        return push(dqs.at[0], dqr.at[source], d_send.at[0], d_recv.at[source], dev(xx, z, c), gg)

    @pl.when(me != 0)
    def _():
        pl.semaphore_wait(far_sem, 1)

    for r in range(1, 2 * heads):
        d_copy(r).start()
    dqr[column] = dqs[flat]
    send_both(jnp.int32(7))
    for h in range(2):
        g_copy(14 + h).wait_recv()

    def final(h, p):
        for way in range(2):
            r_copy(way, 6 + h, p).wait_recv()
        terms = part[8, h, p] + sibr[14 + h, p].astype(F32)
        return (terms + rcv[0, 6 + h, p].astype(F32) + rcv[1, 6 + h, p].astype(F32)).astype(BF16)

    def xr_copy(p):
        return push(xs.at[p], xr.at[p], xr_send.at[p], xr_recv.at[p], across)

    outs = (dv_ref, dk_ref)
    for p in range(2):
        xs[p] = final(0, p)
        xr_copy(p).start()
    for p in range(2):
        outs[p][:, pl.ds(mine, 128)] = final(1, p)
    for r in range(1, 2 * heads):
        d_wait(r).wait_recv()
    for n in range(2 * heads):
        dq_ref[:, n * 128 : (n + 1) * 128] = dqr[n]

    for way in range(2):
        for p in range(PIECES):
            z_copy(way, me, 0, p).wait_send()
            z_copy(way, partner, 1, p).wait_send()

    def drain_gather(e, carry):
        for way in range(2):
            for p in range(PIECES):
                if p // 2 != way:
                    z_copy(way, me, e + 2, p).wait_send()
                else:

                    @pl.when(e < 4)
                    def _():
                        z_copy(way, me, e + 2, p).wait_send()

            for p in range(2):
                r_copy(way, e + 2, p).wait_send()
        return carry

    lax.fori_loop(0, 6, drain_gather, 0)

    def drain_sibling(n, carry):
        for p in range(PIECES):
            sib_copy(me, n, p).wait_send()
        g_copy(n).wait_send()
        return carry

    lax.fori_loop(0, 16, drain_sibling, 0)
    for h in range(2):
        r_copy(0, h, 1).wait_send()
        r_copy(1, h, 0).wait_send()
        x_copy(h).wait_send()
        x_copy(2 + h).wait_send()
        q_copy(h).wait_send()
    for r in range(1, 2 * heads):
        d_copy(r).wait_send()
    for p in range(2):
        xr_copy(p).wait_recv()
        outs[p][:, pl.ds(other, 128)] = xr[p]
        xr_copy(p).wait_send()


def store(dq_ref, dk_ref, dv_ref, dq_out, dk_out, dv_out, sems):
    pairs = ((dq_ref, dq_out), (dk_ref, dk_out), (dv_ref, dv_out))
    copies = [pltpu.make_async_copy(src, dst, sems.at[n]) for n, (src, dst) in enumerate(pairs)]
    for copy in copies:
        copy.start()
    for copy in copies:
        copy.wait()


def local(query_rows, key_rows, value_rows, grad_output, positions):
    rows, width = query_rows.shape
    heads = lax.axis_size("head")
    members = lax.axis_size("seq")
    vmem = pl.BlockSpec(memory_space=pltpu.VMEM)
    dma, tall = pltpu.SemaphoreType.DMA, 2 * rows + 8
    few = rows // heads
    held = pl.pallas_call(
        kernel,
        out_shape=(
            pltpu.VMEM((few, heads * width), BF16),
            pltpu.VMEM((rows, width), BF16),
            pltpu.VMEM((rows, width), BF16),
        ),
        in_specs=[pl.BlockSpec(memory_space=pl.ANY)] * 5,
        out_specs=(vmem,) * 3,
        scratch_shapes=[
            pltpu.VMEM((members, tall, 128), BF16),
            pltpu.VMEM((tall, 128), BF16),
            pltpu.VMEM((2, rows, 128), BF16),
            pltpu.VMEM((2 * rows, 128), BF16),
            pltpu.VMEM((2 * rows, 128), BF16),
            pltpu.VMEM((1, rows), jnp.int32),
            pltpu.VMEM((8, 128), F32),
            pltpu.VMEM((members, rows, 2 * rows), F32),
            pltpu.VMEM((members, rows, 2 * rows), F32),
            pltpu.VMEM((8, 2 * rows), F32),
            pltpu.VMEM((8, 2 * rows), F32),
            pltpu.VMEM((8, 2 * rows), F32),
            pltpu.VMEM((8, 2 * rows), F32),
            pltpu.VMEM((128, 2 * rows), F32),
            pltpu.VMEM((16, 2, rows, 128), BF16),
            pltpu.VMEM((16, 2, rows, 128), BF16),
            pltpu.VMEM((9, 2, 2, rows, 128), F32),
            pltpu.VMEM((2, 8, 2, rows, 128), BF16),
            pltpu.VMEM((2, 8, 2, rows, 128), BF16),
            pltpu.VMEM((2, rows, 128), BF16),
            pltpu.VMEM((2, rows, 128), BF16),
            pltpu.VMEM((2 * heads, few, 128), BF16),
            pltpu.VMEM((2 * heads, few, 128), BF16),
            dma((9,)),
            dma((members, PIECES)),
            dma((2, 8, PIECES)),
            dma((16, PIECES)),
            dma((PIECES + 2,)),
            dma((2,)),
            dma((16,)),
            dma((16,)),
            dma((2, 8, 2)),
            dma((2, 8, 2)),
            dma((2,)),
            dma((2,)),
            dma((2 * heads,)),
            dma((2 * heads,)),
            pltpu.SemaphoreType.REGULAR,
            pltpu.SemaphoreType.REGULAR,
        ],
        compiler_params=pltpu.CompilerParams(
            collective_id=0, has_side_effects=True, vmem_limit_bytes=60 * 1024 * 1024
        ),
    )(query_rows, key_rows, value_rows, grad_output, positions.reshape(1, rows))
    held = [pltpu.with_memory_space_constraint(h, pltpu.VMEM) for h in held]
    return pl.pallas_call(
        store,
        out_shape=tuple(jax.ShapeDtypeStruct(h.shape, h.dtype) for h in held),
        in_specs=[vmem] * 3,
        out_specs=(pl.BlockSpec(memory_space=pl.ANY),) * 3,
        scratch_shapes=[dma((3,))],
    )(*held)


def solution(mesh):
    placed = (P("seq", "head"), P("seq", "head"), P("seq", "head"), P("seq", "head"), P("seq"))
    return jax.shard_map(
        local,
        mesh=mesh,
        in_specs=placed,
        out_specs=(P(("seq", "head"), None), P("seq", "head"), P("seq", "head")),
        check_vma=False,
    )
```

```python
import math

import jax
import jax.numpy as jnp
from jax import lax
from jax.experimental import pallas as pl
from jax.experimental.pallas import tpu as pltpu
from jax.sharding import PartitionSpec as P

MESH = pl.DeviceIdType.MESH
HEAD_DIM = 128
SCALE = HEAD_DIM**-0.5
SCALE2 = SCALE * math.log2(math.e)
FAR = -1e30
Z = 8
PIECES = 4
F32, BF16 = jnp.float32, jnp.bfloat16
NT = (((1,), (1,)), ((), ()))
TN = (((0,), (0,)), ((), ()))


def kernel(
    q_ref, k_ref, v_ref, g_ref, pos_ref, dq_ref, dk_ref, dv_ref,
    kvg, xkv, xq, qf, gf, posr, posb, st, dpt, qpos, mx, tot, dsum, dqt,
    sibs, sibr, part, snd, rcv, xs, xr, dqs, dqr,
    l_sem, in_recv, z_send, sib_send, x_send, q_recv, g_send, g_recv,
    r_send, r_recv, xr_send, xr_recv, d_send, d_recv, go_sem, far_sem,
):
    rows = q_ref.shape[0]
    me, hd = lax.axis_index("seq"), lax.axis_index("head")
    heads = lax.axis_size("head")
    x, z, c = lax.div(me, 16), lax.div(lax.rem(me, 16), 2), lax.rem(me, 2)

    def dev(xx, zz, cc):
        return xx * 16 + zz * 2 + cc

    up, down = dev(x, lax.rem(z + 1, Z), c), dev(x, lax.rem(z + Z - 1, Z), c)
    sibling, across = dev(x, z, 1 - c), dev(1 - x, z, c)
    partner = across

    def push(src, dst, send, recv, seq, head=hd):
        return pltpu.make_async_remote_copy(
            src_ref=src, dst_ref=dst, send_sem=send, recv_sem=recv,
            device_id={"seq": seq, "head": head}, device_id_type=MESH,
        )

    vals, keys, tail = pl.ds(0, rows), pl.ds(rows, rows), pl.ds(2 * rows, 8)
    some = rows // 2
    cut = (pl.ds(0, some), pl.ds(some, some), pl.ds(rows, some), pl.ds(rows + some, some + 8))

    mine, other = pl.multiple_of(x * 128, 128), pl.multiple_of((1 - x) * 128, 128)
    held = pl.ds(pl.multiple_of(x * rows, rows), rows)
    loads = [
        pltpu.make_async_copy(src, dst, l_sem.at[n])
        for n, (src, dst) in enumerate((
            (pos_ref, posr),
            (v_ref.at[:, pl.ds(mine, 128)], kvg.at[me, vals]),
            (v_ref.at[:, pl.ds(other, 128)], xkv.at[vals]),
            (k_ref.at[:, pl.ds(mine, 128)], kvg.at[me, keys]),
            (k_ref.at[:, pl.ds(other, 128)], xkv.at[keys]),
            (q_ref.at[:, pl.ds(other, 128)], xq.at[0]),
            (g_ref.at[:, pl.ds(other, 128)], xq.at[1]),
            (q_ref.at[:, pl.ds(mine, 128)], qf.at[held]),
            (g_ref.at[:, pl.ds(mine, 128)], gf.at[held]),
        ))
    ]
    for load in loads:
        load.start()

    flat = x * heads + hd

    def peer(r):
        there = lax.rem(flat + r, 2 * heads)
        return lax.div(there, heads), lax.rem(there, heads)

    barrier = pltpu.get_barrier_semaphore()

    def signal(sem, seq, head=hd):
        pl.semaphore_signal(sem, inc=1, device_id={"seq": seq, "head": head}, device_id_type=MESH)

    near_by = (up, down, across, sibling)
    for seq in near_by:

        @pl.when(seq != 0)
        def _():
            signal(barrier, seq)

    mx[...] = jnp.full(mx.shape, FAR, F32)
    tot[...] = jnp.zeros(tot.shape, F32)
    dsum[...] = jnp.zeros(dsum.shape, F32)
    dqt[...] = jnp.zeros(dqt.shape, F32)

    loads[0].wait()
    place = posr[...].astype(F32)
    high = jnp.floor(place * (1.0 / 64.0))
    low = place - 64.0 * high
    posb[...] = jnp.zeros(posb.shape, F32)
    for n, digit in enumerate((high, low)):
        posb[2 * n : 2 * n + 1, :] = digit[:, 0:128]
        posb[2 * n + 1 : 2 * n + 2, 0 : rows - 128] = digit[:, 128:rows]
    kvg[me, tail] = posb[...].astype(BF16)
    xkv[tail] = posb[...].astype(BF16)

    @pl.when(me != 0)
    def _():
        pl.semaphore_wait(barrier, 4)
        for seq in near_by:

            @pl.when(seq == 0)
            def _():
                signal(go_sem, seq)

    @pl.when(me == 0)
    def _():
        pl.semaphore_wait(go_sem, 4)

    def z_copy(way, s, n, p):
        return push(kvg.at[s, cut[p]], kvg.at[s, cut[p]], z_send.at[way, n, p], in_recv.at[s, p], (up, down)[way])

    def sib_copy(s, n, p):
        return push(kvg.at[s, cut[p]], kvg.at[s, cut[p]], sib_send.at[n, p], in_recv.at[s, p], sibling)

    def x_copy(p):
        return push(xkv.at[cut[p]], kvg.at[me, cut[p]], x_send.at[p], in_recv.at[me, p], across)

    def q_copy(n):
        return push(xq.at[n], (qf, gf)[n].at[held], x_send.at[4 + n], q_recv.at[n], across)

    for half in range(2):
        loads[1 + 2 * half].wait()
        for p in (2 * half, 2 * half + 1):
            z_copy(0, me, 0, p).start()
            z_copy(1, me, 0, p).start()
        loads[2 + 2 * half].wait()
        for p in (2 * half, 2 * half + 1):
            x_copy(p).start()
        for p in (2 * half, 2 * half + 1):
            sib_copy(me, 0, p).start()
    for n in range(2):
        loads[5 + n].wait()
        q_copy(n).start()

    def arrive(s, p):
        sib_copy(s, 0, p).wait_recv()

    def key_positions(s):
        block = kvg[s, 2 * rows : 2 * rows + 8].astype(F32)
        first = block[0:1] * 64.0 + block[2:3]
        rest = block[1:2] * 64.0 + block[3:4]
        return jnp.concatenate(
            [jnp.broadcast_to(first, (128, 128)).T, jnp.broadcast_to(rest, (128, 128)).T[0 : rows - 128]], axis=0
        )

    def scores(s):
        raw = lax.dot_general(kvg[s, keys], qf[...], NT, preferred_element_type=F32)
        grad_probs = lax.dot_general(kvg[s, vals], gf[...], NT, preferred_element_type=F32)
        columns = key_positions(s)
        columns = jnp.concatenate([columns] * (2 * rows // 128), axis=1)
        raw = jnp.where(columns <= qpos[0:1], raw, FAR)
        st[s] = raw
        dpt[s] = grad_probs
        before = mx[0:1]
        top = jnp.maximum(before, jnp.max(raw, axis=0, keepdims=True))
        fade = jnp.exp2((before - top) * SCALE2)
        p = jnp.exp2((raw - top) * SCALE2)
        mx[0:1] = top
        tot[0:1] = tot[0:1] * fade + jnp.sum(p, axis=0, keepdims=True)
        dsum[0:1] = dsum[0:1] * fade + jnp.sum(p * grad_probs, axis=0, keepdims=True)

    def side(kind):
        return x + kind - 2 * x * kind

    def at(way, far):
        return lax.rem(z + Z - far, Z) if way == 0 else lax.rem(z + far, Z)

    def sib_number(way, e):
        return 2 + 6 * way + e

    def pass_on(e):
        far, kind = lax.div(e, 2) + 1, lax.rem(e, 2)
        for p in range(PIECES):
            for way in range(2):
                s = dev(side(kind), at(way, far), c)
                arrive(s, p)
                if p // 2 != way:
                    z_copy(way, s, e + 2, p).start()
                else:

                    @pl.when(far <= 2)
                    def _():
                        z_copy(way, s, e + 2, p).start()

                sib_copy(s, sib_number(way, e), p).start()

    def arrive_whole(s):
        for p in range(PIECES):
            arrive(s, p)

    def score_own(e):
        far, kind = lax.div(e, 2) + 1, lax.rem(e, 2)
        for way in range(2):
            scores(dev(side(kind), at(way, far), c))

    def score_sibling(e):
        far, kind = lax.div(e, 2) + 1, lax.rem(e, 2)
        for way in range(2):
            s = dev(side(kind), at(way, far), 1 - c)
            arrive_whole(s)
            scores(s)

    for p in range(PIECES):
        arrive(partner, p)
        z_copy(0, partner, 1, p).start()
        z_copy(1, partner, 1, p).start()
        sib_copy(partner, 1, p).start()
    pass_on(jnp.int32(0))
    for n in range(2):
        loads[7 + n].wait()
        q_copy(n).wait_recv()
    both = jnp.concatenate([key_positions(dev(0, z, c)), key_positions(dev(1, z, c))], axis=0)
    qpos[...] = both.T[0:8]

    def near(kind, carry):
        scores(dev(kind, z, c))
        return carry

    def near_sibling(kind, carry):
        s = dev(side(kind), z, 1 - c)
        arrive_whole(s)
        scores(s)
        return carry

    lax.fori_loop(0, 2, near, 0)
    lax.fori_loop(0, 2, near_sibling, 0)

    def gather_step(e, carry):
        pass_on(e)
        score_own(e - 1)
        score_sibling(e - 1)
        return carry

    lax.fori_loop(1, 6, gather_step, 0)

    def far_pass(kind):
        for p in (2, 0, 3, 1):
            s = dev(side(kind), at(0, 4), c)
            arrive(s, p)
            sib_copy(s, 14 + kind, p).start()

    def far_own(kind, carry):
        scores(dev(side(kind), at(0, 4), c))
        return carry

    def far_sibling(kind, carry):
        s = dev(side(kind), at(0, 4), 1 - c)
        arrive_whole(s)
        scores(s)
        return carry

    far_pass(0)
    score_own(jnp.int32(5))
    score_sibling(jnp.int32(5))
    far_pass(1)
    lax.fori_loop(0, 2, far_own, 0)
    lax.fori_loop(0, 2, far_sibling, 0)

    @pl.when(me == 0)
    def _():
        for r in range(1, heads):
            signal(barrier, me, lax.rem(hd + r, heads))

    total = tot[0:1]
    mx[0:1] = mx[0:1] * SCALE2 + jnp.log2(total)
    dsum[0:1] = dsum[0:1] / total

    def grads(s):
        p = jnp.exp2(st[s] * SCALE2 - mx[0:1])
        grad_scores = (p * (dpt[s] - dsum[0:1])).astype(BF16)
        dv = jnp.dot(p.astype(BF16), gf[...], preferred_element_type=F32)
        dk = jnp.dot(grad_scores, qf[...], preferred_element_type=F32) * SCALE
        dqt[...] += lax.dot_general(kvg[s, keys], grad_scores, TN, preferred_element_type=F32)
        return dv, dk

    def g_copy(n):
        return push(sibs.at[n], sibr.at[n], g_send.at[n], g_recv.at[n], sibling)

    def r_copy(way, h, p):
        return push(snd.at[way, h, p], rcv.at[way, h, p], r_send.at[way, h, p], r_recv.at[way, h, p], (up, down)[way])

    def for_sibling(s, n):
        for p, term in enumerate(grads(s)):
            sibs[n, p] = term.astype(BF16)
        g_copy(n).start()

    def for_own(s, h, way):
        for p, term in enumerate(grads(s)):
            part[h, way, p] = term

    def farthest_sibling(h, carry):
        for_sibling(dev(side(1 - h), at(1, 4), 1 - c), h)
        return carry

    def farthest(h, carry):
        for_own(dev(side(1 - h), at(1, 4), c), h, 0)
        g_copy(h).wait_recv()
        for way in range(2):
            p = 1 - way
            snd[way, h, p] = (part[h, 0, p] + sibr[h, p].astype(F32)).astype(BF16)
            r_copy(way, h, p).start()
        return carry

    lax.fori_loop(0, 2, farthest_sibling, 0)
    lax.fori_loop(0, 2, farthest, 0)

    def step_terms(h):
        far = 4 - lax.div(h, 2)
        for way in range(2):
            xx = side(jnp.where(h == 8, 1 - way, 1 - lax.rem(h, 2)))
            for_sibling(dev(xx, at(1 - way, far), 1 - c), 2 * h - 2 + way)
        for way in range(2):
            xx = side(jnp.where(h == 8, 1 - way, 1 - lax.rem(h, 2)))
            for_own(dev(xx, at(1 - way, far), c), h, way)

    def here(h, way, p):
        return part[h, way, p] + sibr[2 * h - 2 + way, p].astype(F32)

    def send_first(h):
        for way in range(2):
            g_copy(2 * h - 2 + way).wait_recv()
            snd[way, h, way] = here(h, way, way).astype(BF16)
            r_copy(way, h, way).start()

    def send_summed(h, turn):
        for way in range(2):
            p = turn if way == 0 else 1 - turn
            r_copy(way, h - 2, p).wait_recv()
            snd[way, h, p] = (here(h, way, p) + rcv[way, h - 2, p].astype(F32)).astype(BF16)
            r_copy(way, h, p).start()

    def send_both(h):
        for way in range(2):
            g_copy(2 * h - 2 + way).wait_recv()
        send_summed(h, 0)
        send_summed(h, 1)

    def first_step(h, carry):
        step_terms(h)
        send_first(h)
        return carry

    lax.fori_loop(2, 4, first_step, 0)

    def reduce_step(h, carry):
        @pl.when(jnp.logical_and(h == 6, me == 0))
        def _():
            pl.semaphore_wait(barrier, heads - 1)

            def tell(n, carry):
                signal(far_sem, n)
                return carry

            lax.fori_loop(1, lax.axis_size("seq"), tell, 0)

        step_terms(h)

        @pl.when(h == 4)
        def _():
            send_summed(jnp.int32(2), 1)
            send_summed(jnp.int32(3), 1)

        @pl.when(jnp.logical_and(h > 4, h < 8))
        def _():
            send_both(h - 1)

        return carry

    lax.fori_loop(4, 9, reduce_step, 0)

    grad_query = dqt[...].T * SCALE
    few = rows // heads
    for n in range(2 * heads):
        dqs[n] = grad_query[n * few : (n + 1) * few].astype(BF16)
    column = hd * 2 + x

    def d_copy(r):
        xx, gg = peer(r)
        n = xx * heads + gg
        return push(dqs.at[n], dqr.at[column], d_send.at[n], d_recv.at[column], dev(xx, z, c), gg)

    def d_wait(r):
        xx, gg = peer(r)
        source = gg * 2 + xx
        return push(dqs.at[0], dqr.at[source], d_send.at[0], d_recv.at[source], dev(xx, z, c), gg)

    @pl.when(me != 0)
    def _():
        pl.semaphore_wait(far_sem, 1)

    for r in range(1, 2 * heads):
        d_copy(r).start()
    dqr[column] = dqs[flat]
    send_both(jnp.int32(7))
    for h in range(2):
        g_copy(14 + h).wait_recv()

    def final(h, p):
        for way in range(2):
            r_copy(way, 6 + h, p).wait_recv()
        terms = part[8, h, p] + sibr[14 + h, p].astype(F32)
        return (terms + rcv[0, 6 + h, p].astype(F32) + rcv[1, 6 + h, p].astype(F32)).astype(BF16)

    def xr_copy(p):
        return push(xs.at[p], xr.at[p], xr_send.at[p], xr_recv.at[p], across)

    outs = (dv_ref, dk_ref)
    for p in range(2):
        xs[p] = final(0, p)
        xr_copy(p).start()
    for p in range(2):
        outs[p][:, pl.ds(mine, 128)] = final(1, p)
    for r in range(1, 2 * heads):
        d_wait(r).wait_recv()
    for n in range(2 * heads):
        dq_ref[:, n * 128 : (n + 1) * 128] = dqr[n]

    for way in range(2):
        for p in range(PIECES):
            z_copy(way, me, 0, p).wait_send()
            z_copy(way, partner, 1, p).wait_send()

    def drain_gather(e, carry):
        for way in range(2):
            for p in range(PIECES):
                if p // 2 != way:
                    z_copy(way, me, e + 2, p).wait_send()
                else:

                    @pl.when(e < 4)
                    def _():
                        z_copy(way, me, e + 2, p).wait_send()

            for p in range(2):
                r_copy(way, e + 2, p).wait_send()
        return carry

    lax.fori_loop(0, 6, drain_gather, 0)

    def drain_sibling(n, carry):
        for p in range(PIECES):
            sib_copy(me, n, p).wait_send()
        g_copy(n).wait_send()
        return carry

    lax.fori_loop(0, 16, drain_sibling, 0)
    for h in range(2):
        r_copy(0, h, 1).wait_send()
        r_copy(1, h, 0).wait_send()
        x_copy(h).wait_send()
        x_copy(2 + h).wait_send()
        q_copy(h).wait_send()
    for r in range(1, 2 * heads):
        d_copy(r).wait_send()
    for p in range(2):
        xr_copy(p).wait_recv()
        outs[p][:, pl.ds(other, 128)] = xr[p]
        xr_copy(p).wait_send()


def store(dq_ref, dk_ref, dv_ref, dq_out, dk_out, dv_out, sems):
    pairs = ((dq_ref, dq_out), (dk_ref, dk_out), (dv_ref, dv_out))
    copies = [pltpu.make_async_copy(src, dst, sems.at[n]) for n, (src, dst) in enumerate(pairs)]
    for copy in copies:
        copy.start()
    for copy in copies:
        copy.wait()


def local(query_rows, key_rows, value_rows, grad_output, positions):
    rows, width = query_rows.shape
    heads = lax.axis_size("head")
    members = lax.axis_size("seq")
    vmem = pl.BlockSpec(memory_space=pltpu.VMEM)
    dma, tall = pltpu.SemaphoreType.DMA, 2 * rows + 8
    few = rows // heads
    held = pl.pallas_call(
        kernel,
        out_shape=(
            pltpu.VMEM((few, heads * width), BF16),
            pltpu.VMEM((rows, width), BF16),
            pltpu.VMEM((rows, width), BF16),
        ),
        in_specs=[pl.BlockSpec(memory_space=pl.ANY)] * 5,
        out_specs=(vmem,) * 3,
        scratch_shapes=[
            pltpu.VMEM((members, tall, 128), BF16),
            pltpu.VMEM((tall, 128), BF16),
            pltpu.VMEM((2, rows, 128), BF16),
            pltpu.VMEM((2 * rows, 128), BF16),
            pltpu.VMEM((2 * rows, 128), BF16),
            pltpu.VMEM((1, rows), jnp.int32),
            pltpu.VMEM((8, 128), F32),
            pltpu.VMEM((members, rows, 2 * rows), F32),
            pltpu.VMEM((members, rows, 2 * rows), F32),
            pltpu.VMEM((8, 2 * rows), F32),
            pltpu.VMEM((8, 2 * rows), F32),
            pltpu.VMEM((8, 2 * rows), F32),
            pltpu.VMEM((8, 2 * rows), F32),
            pltpu.VMEM((128, 2 * rows), F32),
            pltpu.VMEM((16, 2, rows, 128), BF16),
            pltpu.VMEM((16, 2, rows, 128), BF16),
            pltpu.VMEM((9, 2, 2, rows, 128), F32),
            pltpu.VMEM((2, 8, 2, rows, 128), BF16),
            pltpu.VMEM((2, 8, 2, rows, 128), BF16),
            pltpu.VMEM((2, rows, 128), BF16),
            pltpu.VMEM((2, rows, 128), BF16),
            pltpu.VMEM((2 * heads, few, 128), BF16),
            pltpu.VMEM((2 * heads, few, 128), BF16),
            dma((9,)),
            dma((members, PIECES)),
            dma((2, 8, PIECES)),
            dma((16, PIECES)),
            dma((PIECES + 2,)),
            dma((2,)),
            dma((16,)),
            dma((16,)),
            dma((2, 8, 2)),
            dma((2, 8, 2)),
            dma((2,)),
            dma((2,)),
            dma((2 * heads,)),
            dma((2 * heads,)),
            pltpu.SemaphoreType.REGULAR,
            pltpu.SemaphoreType.REGULAR,
        ],
        compiler_params=pltpu.CompilerParams(
            collective_id=0, has_side_effects=True, vmem_limit_bytes=60 * 1024 * 1024
        ),
    )(query_rows, key_rows, value_rows, grad_output, positions.reshape(1, rows))
    held = [pltpu.with_memory_space_constraint(h, pltpu.VMEM) for h in held]
    return pl.pallas_call(
        store,
        out_shape=tuple(jax.ShapeDtypeStruct(h.shape, h.dtype) for h in held),
        in_specs=[vmem] * 3,
        out_specs=(pl.BlockSpec(memory_space=pl.ANY),) * 3,
        scratch_shapes=[dma((3,))],
    )(*held)


def solution(mesh):
    placed = (P("seq", "head"), P("seq", "head"), P("seq", "head"), P("seq", "head"), P("seq"))
    return jax.shard_map(
        local,
        mesh=mesh,
        in_specs=placed,
        out_specs=(P(("seq", "head"), None), P("seq", "head"), P("seq", "head")),
        check_vma=False,
    )
```
